8 devices in a mesh: dp: 1 (over z), tp: 2 (over y), sp: 4 (over x, core).
Axes of the slice: x: 2, y: 2, z: 1, core: 2. Of those that a mesh axis runs over, the one named last changes fastest.
Arguments:
- tokens: bfloat16 [16, 6144], P(('dp', 'sp'))
- states: float32 [4, 16, 64, 128, 128], P('sp', 'dp', 'tp')
- k_cache: bfloat16 [16, 8, 4096, 128], P('dp', 'tp', 'sp')
- v_cache: bfloat16 [16, 8, 4096, 128], P('dp', 'tp', 'sp')
- slopes: float32 [64], P('tp')
- lin_gain: float32 [6144], replicated
- w_lin_qkv: bfloat16 [6144, 3, 8192], P(None, None, 'tp')
- w_lin_gate: bfloat16 [6144, 8192], P(None, 'tp')
- out_gain: float32 [8192], P('tp')
- w_lin_out: bfloat16 [8192, 6144], P('tp')
- attn_gain: float32 [6144], replicated
- w_attn_in: bfloat16 [6144, 8, 10, 128], P(None, 'tp')
- w_attn_out: bfloat16 [8192, 6144], P('tp')
Outputs:
- output 1: bfloat16 [16, 6144], P(('dp', 'sp'))
- output 2: float32 [16, 64, 128, 128], P(('dp', 'sp'), 'tp')
- output 3: bfloat16 [16, 8, 4112, 128], P(('dp', 'sp'), 'tp')
- output 4: bfloat16 [16, 8, 4112, 128], P(('dp', 'sp'), 'tp')
All inputs are finite; a program needn't handle non-finite values.
Results may differ from the reference program's by a relative error of at most 0.0124783.
Values are sent between devices in bfloat16 or wider.
A program may use at most 2 GiB of HBM per device.

```python
import jax
import jax.numpy as jnp
from jax import lax

MODEL_DIM = 6144
NUM_HEADS = 64
KV_COUNT = 8
HEAD_DIM = 128
SEQ_SHARDS = 4
BATCH = 16
SHARD_LEN = 1024
CACHE_EXTRA = 16

PROMPT_LEN = SEQ_SHARDS * SHARD_LEN
HIDDEN = NUM_HEADS * HEAD_DIM
GROUP = NUM_HEADS // KV_COUNT
ROPE_DIM = HEAD_DIM // 2
NORM_EPS = 1e-6
ROPE_BASE = 10000000.0
RES_ALPHA = 1.0
RES_BETA = 1.0


def draw_weight(key, shape, fan_in):
    return (jax.random.normal(key, shape, jnp.float32) * fan_in ** -0.5).astype(jnp.bfloat16)


def draw_gain(key, width):
    return 1.0 + 0.3 * jax.random.normal(key, (width,), jnp.float32)


def draw_cache(key, wave_cos, wave_sin):
    sub_keys = jax.random.split(key, 3)
    amplitude = jax.random.normal(sub_keys[0], (BATCH, KV_COUNT, 3, HEAD_DIM), jnp.float32) * (2.0 / 3.0) ** 0.5
    phases = jax.random.uniform(sub_keys[1], (BATCH, KV_COUNT, 3, HEAD_DIM), jnp.float32, 0.0, 2.0 * jnp.pi)
    slow_part = jnp.einsum('bkjd,jt->bktd', amplitude * jnp.cos(phases), wave_cos) - jnp.einsum('bkjd,jt->bktd', amplitude * jnp.sin(phases), wave_sin)
    noise_vals = jax.random.normal(sub_keys[2], (BATCH, KV_COUNT, PROMPT_LEN, HEAD_DIM), jnp.float32)
    return (slow_part + 0.5 * noise_vals).astype(jnp.bfloat16)


def setup_inputs(seed: int = 0, part: int = 0) -> dict:
    base_key = jax.random.key(seed)
    shared = jax.random.split(base_key, 12)
    own_keys = jax.random.split(jax.random.fold_in(base_key, part), 4)
    positions = jnp.arange(PROMPT_LEN, dtype=jnp.float32) / PROMPT_LEN
    wave_arg = 2.0 * jnp.pi * jnp.arange(1, 4, dtype=jnp.float32)[:, None] * positions[None, :]
    wave_cos = jnp.cos(wave_arg)
    wave_sin = jnp.sin(wave_arg)
    return {
        'tokens': jax.random.normal(own_keys[0], (BATCH, MODEL_DIM), jnp.float32).astype(jnp.bfloat16),
        'states': jax.random.normal(own_keys[1], (SEQ_SHARDS, BATCH, NUM_HEADS, HEAD_DIM, HEAD_DIM), jnp.float32),
        'k_cache': draw_cache(own_keys[2], wave_cos, wave_sin),
        'v_cache': draw_cache(own_keys[3], wave_cos, wave_sin),
        'slopes': jax.random.uniform(shared[0], (NUM_HEADS,), jnp.float32, 0.2, 1.2) / PROMPT_LEN,
        'lin_gain': draw_gain(shared[1], MODEL_DIM),
        'w_lin_qkv': draw_weight(shared[2], (MODEL_DIM, 3, HIDDEN), MODEL_DIM),
        'w_lin_gate': draw_weight(shared[3], (MODEL_DIM, HIDDEN), MODEL_DIM),
        'out_gain': draw_gain(shared[4], HIDDEN),
        'w_lin_out': draw_weight(shared[5], (HIDDEN, MODEL_DIM), HIDDEN),
        'attn_gain': draw_gain(shared[6], MODEL_DIM),
        'w_attn_in': draw_weight(shared[7], (MODEL_DIM, KV_COUNT, GROUP + 2, HEAD_DIM), MODEL_DIM),
        'w_attn_out': draw_weight(shared[8], (HIDDEN, MODEL_DIM), HIDDEN),
    }


def rms_norm(vals_in, gain_vec):
    vals32 = vals_in.astype(jnp.float32)
    inv_rms = lax.rsqrt(jnp.mean(vals32 * vals32, axis=-1, keepdims=True) + NORM_EPS)
    return vals32 * inv_rms * gain_vec


def rotary(vals_in):
    half_dim = ROPE_DIM // 2
    inv_freq = ROPE_BASE ** (-jnp.arange(0, ROPE_DIM, 2, dtype=jnp.float32) / ROPE_DIM)
    angles = PROMPT_LEN * inv_freq
    cosine = jnp.cos(angles)
    sine_vals = jnp.sin(angles)
    vals32 = vals_in.astype(jnp.float32)
    first_half = vals32[..., :half_dim]
    second_half = vals32[..., half_dim:ROPE_DIM]
    return jnp.concatenate([first_half * cosine - second_half * sine_vals, second_half * cosine + first_half * sine_vals, vals32[..., ROPE_DIM:]], axis=-1).astype(jnp.bfloat16)


def attend_row(row_data):
    query_rot, keys_row, values_row, key_new, value_new = row_data
    score_scale = HEAD_DIM ** -0.5
    query_f32 = query_rot.astype(jnp.float32)
    scores = jnp.einsum('kgd,ktd->kgt', query_f32, keys_row.astype(jnp.float32)) * score_scale
    new_score = jnp.einsum('kgd,kd->kg', query_f32, key_new.astype(jnp.float32)) * score_scale
    row_max = jnp.maximum(jnp.max(scores, axis=-1), new_score)
    probs = jnp.exp(scores - row_max[..., None])
    new_prob = jnp.exp(new_score - row_max)
    prob_sum = jnp.sum(probs, axis=-1) + new_prob
    weighted_sum = jnp.einsum('kgt,ktd->kgd', probs.astype(jnp.bfloat16).astype(jnp.float32), values_row.astype(jnp.float32))
    weighted_sum = weighted_sum + new_prob.astype(jnp.bfloat16).astype(jnp.float32)[..., None] * value_new.astype(jnp.float32)[:, None, :]
    return weighted_sum / prob_sum[..., None]


def reference(tokens, states, k_cache, v_cache, slopes, lin_gain, w_lin_qkv, w_lin_gate, out_gain, w_lin_out, attn_gain, w_attn_in, w_attn_out):
    normed = rms_norm(tokens, lin_gain).astype(jnp.bfloat16)
    offsets = (SHARD_LEN * (SEQ_SHARDS - 1 - jnp.arange(SEQ_SHARDS))).astype(jnp.float32)
    shard_weight = jnp.exp(-slopes[None, :] * offsets[:, None])
    moved_state = jnp.einsum('ch,cbhde->bhde', shard_weight, states)
    lin_proj = jnp.dot(normed, w_lin_qkv.reshape(MODEL_DIM, 3 * HIDDEN), preferred_element_type=jnp.float32)
    act_vals = jax.nn.silu(lin_proj).astype(jnp.bfloat16).reshape(BATCH, 3, NUM_HEADS, HEAD_DIM).astype(jnp.float32)
    state_new = jnp.exp(-slopes)[None, :, None, None] * moved_state + jnp.einsum('bhd,bhe->bhde', act_vals[:, 1], act_vals[:, 2])
    lin_attn = jnp.einsum('bhd,bhde->bhe', act_vals[:, 0], state_new).reshape(BATCH, HIDDEN)
    gate_vals = jax.nn.sigmoid(jnp.dot(normed, w_lin_gate, preferred_element_type=jnp.float32))
    mixed_out = (rms_norm(lin_attn, out_gain) * gate_vals).astype(jnp.bfloat16)
    lin_out = jnp.dot(mixed_out, w_lin_out, preferred_element_type=jnp.float32)
    hidden = (RES_ALPHA * normed.astype(jnp.float32) + RES_BETA * lin_out).astype(jnp.bfloat16)

    normed_two = rms_norm(hidden, attn_gain).astype(jnp.bfloat16)
    attn_proj = jnp.dot(normed_two, w_attn_in.reshape(MODEL_DIM, KV_COUNT * (GROUP + 2) * HEAD_DIM), preferred_element_type=jnp.float32)
    attn_proj = attn_proj.astype(jnp.bfloat16).reshape(BATCH, KV_COUNT, GROUP + 2, HEAD_DIM)
    query_rot = rotary(attn_proj[:, :, :GROUP])
    key_new = rotary(attn_proj[:, :, GROUP])
    value_new = attn_proj[:, :, GROUP + 1]
    head_out = lax.map(attend_row, (query_rot, k_cache, v_cache, key_new, value_new))
    attn_out = jnp.dot(head_out.astype(jnp.bfloat16).reshape(BATCH, HIDDEN), w_attn_out, preferred_element_type=jnp.float32)
    hidden_out = (RES_ALPHA * normed_two.astype(jnp.float32) + RES_BETA * attn_out).astype(jnp.bfloat16)
    tail_zeros = jnp.zeros((BATCH, KV_COUNT, CACHE_EXTRA - 1, HEAD_DIM), jnp.bfloat16)
    k_out = jnp.concatenate([k_cache, key_new[:, :, None, :], tail_zeros], axis=2)
    v_out = jnp.concatenate([v_cache, value_new[:, :, None, :], tail_zeros], axis=2)
    return (hidden_out, state_new, k_out, v_out)
```

```python
import jax
import jax.numpy as jnp
from jax import lax
from jax.experimental import pallas as pl
from jax.experimental.pallas import tpu as pltpu
from jax.sharding import PartitionSpec as P


NORM_EPS = 1e-6
ROPE_BASE = 10000000.0
RES_ALPHA = 1.0
RES_BETA = 1.0
CACHE_EXTRA = 16


F32 = jnp.float32
BF16 = jnp.bfloat16


def rms_norm(vals_in, gain_vec):
    vals32 = vals_in.astype(F32)
    inv_rms = lax.rsqrt(jnp.mean(vals32 * vals32, axis=-1, keepdims=True) + NORM_EPS)
    return vals32 * inv_rms * gain_vec


def rotary(vals_in, position):
    rope_dim = vals_in.shape[-1] // 2
    half_dim = rope_dim // 2
    inv_freq = ROPE_BASE ** (-jnp.arange(0, rope_dim, 2, dtype=F32) / rope_dim)
    angles = position * inv_freq
    cosine = jnp.cos(angles)
    sine_vals = jnp.sin(angles)
    vals32 = vals_in.astype(F32)
    first_half = vals32[..., :half_dim]
    second_half = vals32[..., half_dim:rope_dim]
    return jnp.concatenate([first_half * cosine - second_half * sine_vals, second_half * cosine + first_half * sine_vals, vals32[..., rope_dim:]], axis=-1).astype(BF16)


def merge(out_a, stats_a, out_b, stats_b):
    top = jnp.maximum(stats_a[:, 0], stats_b[:, 0])
    scale_a = jnp.exp(stats_a[:, 0] - top)
    scale_b = jnp.exp(stats_b[:, 0] - top)
    total = stats_a[:, 1] * scale_a + stats_b[:, 1] * scale_b
    return out_a * scale_a[..., None] + out_b * scale_b[..., None], jnp.stack([top, total], axis=1)


def pack(out, stats):
    rows, _, heads, group = stats.shape
    tail = jnp.transpose(stats, (2, 3, 0, 1)).reshape(1, heads, group, 2 * rows)
    return jnp.concatenate([out, jnp.pad(tail, ((0, 0), (0, 0), (0, 0), (0, out.shape[-1] - 2 * rows)))])


def unpack(packed):
    rows, heads, group = packed.shape[0] - 1, packed.shape[1], packed.shape[2]
    tail = packed[rows, :, :, :2 * rows].reshape(heads, group, rows, 2)
    return packed[:rows], jnp.transpose(tail, (2, 3, 0, 1))


def place_last_block(src_ref, total_ref, out_ref, buf, in_sems, out_sems):
    heads, length = src_ref.shape[1], src_ref.shape[2]
    row = out_ref.shape[0] - 1
    pos = pl.multiple_of((3 - lax.axis_index('sp')) * length, length)
    reads = [pltpu.make_async_copy(src_ref.at[0, j], buf.at[j], in_sems.at[j]) for j in range(heads)]
    writes = [pltpu.make_async_copy(buf.at[j], out_ref.at[row, j, pl.ds(pos, length)], out_sems.at[j]) for j in range(heads)]
    for copy in reads:
        copy.start()
    for read, write in zip(reads, writes):
        read.wait()
        write.start()
    for copy in writes:
        copy.wait()


def place_last(total, block):
    heads, length, dim = block.shape[1:]
    return pl.pallas_call(
        place_last_block,
        in_specs=[pl.BlockSpec(memory_space=pl.ANY), pl.BlockSpec(memory_space=pl.ANY)],
        out_specs=pl.BlockSpec(memory_space=pl.ANY),
        out_shape=jax.ShapeDtypeStruct(total.shape, total.dtype),
        scratch_shapes=[pltpu.VMEM((heads, length, dim), block.dtype), pltpu.SemaphoreType.DMA((heads,)), pltpu.SemaphoreType.DMA((heads,))],
        input_output_aliases={1: 0},
        compiler_params=pltpu.CompilerParams(vmem_limit_bytes=67043328),
        name="place_last",
    )(block, total)


def copy_block(_, src_ref, *refs):
    refs[-1][...] = src_ref[...]


def place(total, block, first, pos_block, out_shape, count=None, out_first=0):
    rows, heads, _, dim = out_shape
    length = block.shape[2]
    if length > CACHE_EXTRA:
        count = rows if count is None else count
        grid, shape = (count, heads // 2), (1, 2, length, dim)
    else:
        count, grid, shape = rows, (1, 1), (rows, heads, length, dim)
    scalars = jnp.stack([jnp.asarray(first, jnp.int32), jnp.asarray(pos_block, jnp.int32)])
    in_specs = [pl.BlockSpec(shape, lambda i, j, s: (s[0] + i, j, 0, 0))]
    operands = [scalars, block]
    aliases = {}
    if total is not None:
        in_specs.append(pl.BlockSpec(memory_space=pl.ANY))
        operands.append(total)
        aliases = {2: 0}
    nbytes = 2 * count * heads * length * dim * 2
    return pl.pallas_call(
        copy_block,
        grid_spec=pltpu.PrefetchScalarGridSpec(
            num_scalar_prefetch=1,
            grid=grid,
            in_specs=in_specs,
            out_specs=pl.BlockSpec(shape, lambda i, j, s: (out_first + i, j, s[1], 0)),
        ),
        out_shape=jax.ShapeDtypeStruct(out_shape, block.dtype),
        input_output_aliases=aliases,
        compiler_params=pltpu.CompilerParams(vmem_limit_bytes=67043328),
        cost_estimate=pl.CostEstimate(flops=nbytes * 30, bytes_accessed=nbytes, transcendentals=0),
        name="place",
    )(*operands)


def solution(mesh):
    seq_shards = mesh.shape['sp']
    tp_size = mesh.shape['tp']

    def send(value, mask):
        return lax.ppermute(value, 'sp', [(i, i ^ mask) for i in range(seq_shards)])

    def tp_sum(value):
        return value + lax.ppermute(value, 'tp', [(0, 1), (1, 0)])

    def step(tokens, states, k_cache, v_cache, slopes, lin_gain, w_lin_qkv, w_lin_gate, out_gain, w_lin_out, attn_gain, w_attn_in, w_attn_out):
        rows = tokens.shape[0]
        kv_dev = k_cache.shape[1]
        shard_len = k_cache.shape[2]
        head_dim = k_cache.shape[3]
        group = w_attn_in.shape[2] - 2
        heads_dev = slopes.shape[0]
        prompt_len = seq_shards * shard_len
        me = lax.axis_index('sp')

        def rows_of(value, mask, first=0, count=rows):
            return lax.dynamic_slice_in_dim(value, rows * (me ^ mask) + first, count, 0)

        kx0_rows = rows_of(k_cache, 2, 0, 1)
        kx0 = send(kx0_rows, 2)
        k_src, slopes_a = lax.optimization_barrier((k_cache, slopes, kx0_rows))[:2]
        kx1_rows = rows_of(k_src, 2, 1, rows - 1)
        kx1 = send(kx1_rows, 2)

        own = states[0]
        offset = (shard_len * (seq_shards - 1 - me)).astype(F32)
        decay = jnp.exp(-slopes_a * offset)[None, :, None, None]
        sa_rows = rows_of(own, 3) * decay
        sb_rows = rows_of(own, 1) * decay
        sa = send(sa_rows, 1)
        sb = send(sb_rows, 1)

        normed = rms_norm(tokens, lin_gain).astype(BF16)
        lin_proj = jnp.einsum('bd,dkn->bkn', normed, w_lin_qkv, preferred_element_type=F32)
        act_vals = jax.nn.silu(lin_proj).astype(BF16).reshape(rows, 3, heads_dev, head_dim)

        part_x = rows_of(own, 2) * decay + sa
        sx = send(part_x, 2)

        k_src, v_src, _ = lax.optimization_barrier((k_cache, v_cache, part_x))
        ky_rows = rows_of(k_src, 3)
        kd_rows = rows_of(k_src, 1)
        vd_rows = rows_of(v_src, 1)
        vx_rows = rows_of(v_src, 2)
        vy0_rows = rows_of(v_src, 3, 0, rows - 1)
        vy1_rows = rows_of(v_src, 3, rows - 1, 1)
        ky = send(ky_rows, 3)
        kd = send(kd_rows, 1)
        vd = send(vd_rows, 1)

        gate_vals = jax.nn.sigmoid(jnp.dot(normed, w_lin_gate, preferred_element_type=F32))
        gate_vals = lax.optimization_barrier(gate_vals)

        moved_state = rows_of(own, 0) * decay + sb + sx
        state_new = jnp.exp(-slopes)[None, :, None, None] * moved_state + jnp.einsum('bhd,bhe->bhde', act_vals[:, 1], act_vals[:, 2], preferred_element_type=F32)
        lin_attn = jnp.einsum('bhd,bhde->bhe', act_vals[:, 0].astype(F32), state_new).reshape(rows, heads_dev * head_dim)
        square_sum = tp_sum(jnp.sum(lin_attn * lin_attn, axis=-1, keepdims=True))
        inv_rms = lax.rsqrt(square_sum / (tp_size * heads_dev * head_dim) + NORM_EPS)
        mixed_out = (lin_attn * inv_rms * out_gain * gate_vals).astype(BF16)
        lin_out = jnp.dot(mixed_out, w_lin_out, preferred_element_type=F32)
        lin_out = tp_sum(lin_out)
        hidden = (RES_ALPHA * normed.astype(F32) + RES_BETA * lin_out).astype(BF16)
        normed_two = rms_norm(hidden, attn_gain).astype(BF16)
        attn_proj = jnp.einsum('bd,dkjn->bkjn', normed_two, w_attn_in, preferred_element_type=F32).astype(BF16)
        query_rot = rotary(attn_proj[:, :, :group], prompt_len)
        key_new = rotary(attn_proj[:, :, group], prompt_len)
        value_new = attn_proj[:, :, group + 1]

        qx = send(query_rot, 2)
        vx = send(vx_rows, 2)
        qd = send(jnp.stack([query_rot, qx]), 1)

        score_scale = head_dim ** -0.5
        order = jnp.arange(seq_shards) ^ me
        query_all = jnp.take(jnp.stack([query_rot, qd[0], qx, qd[1]]), order, axis=0).reshape(seq_shards * rows, kv_dev, group, head_dim)
        scores = jnp.einsum('bkgd,bktd->bkgt', query_all, k_cache, preferred_element_type=F32) * score_scale
        part_max = jnp.max(scores, axis=-1)
        probs = jnp.exp(scores - part_max[..., None])
        part_sum = jnp.sum(probs, axis=-1)
        part_out = jnp.einsum('bkgt,bktd->bkgd', probs.astype(BF16), v_cache, preferred_element_type=F32)
        stats = jnp.stack([part_max, part_sum], axis=1)

        pair = pack(jnp.concatenate([rows_of(part_out, 3), rows_of(part_out, 1)]), jnp.concatenate([rows_of(stats, 3), rows_of(stats, 1)]))
        pair_out, pair_stats = unpack(send(pair, 1))
        far = pack(*merge(rows_of(part_out, 2), rows_of(stats, 2), pair_out[:rows], pair_stats[:rows]))
        ax, axs = unpack(send(far, 2))
        vy0 = send(vy0_rows, 3)
        vy1 = send(vy1_rows, 3)

        near_out, near_stats = merge(rows_of(part_out, 0), rows_of(stats, 0), pair_out[rows:], pair_stats[rows:])
        all_out, all_stats = merge(near_out, near_stats, ax, axs)
        new_score = jnp.einsum('clhe,cle->clh', query_rot, key_new, preferred_element_type=F32) * score_scale
        row_max = jnp.maximum(all_stats[:, 0], new_score)
        scale = jnp.exp(all_stats[:, 0] - row_max)
        new_prob = jnp.exp(new_score - row_max)
        prob_sum = all_stats[:, 1] * scale + new_prob
        weighted_sum = all_out * scale[..., None]
        weighted_sum = weighted_sum + new_prob.astype(BF16).astype(F32)[..., None] * value_new.astype(F32)[:, :, None, :]
        head_out = (weighted_sum / prob_sum[..., None]).astype(BF16).reshape(rows, kv_dev * group * head_dim)
        attn_out = jnp.dot(head_out, w_attn_out, preferred_element_type=F32)
        attn_out = tp_sum(attn_out)
        hidden_out = (RES_ALPHA * normed_two.astype(F32) + RES_BETA * attn_out).astype(BF16)

        out_shape = (rows, kv_dev, prompt_len + CACHE_EXTRA, head_dim)
        tail_zeros = jnp.zeros((rows, kv_dev, CACHE_EXTRA - 1, head_dim), BF16)
        late, _ = lax.optimization_barrier((me, part_x))

        def add_tail(total, new_row):
            tail = jnp.concatenate([new_row[:, :, None, :], tail_zeros], axis=2)
            return place(total, tail, 0, prompt_len // CACHE_EXTRA, out_shape)

        k_out = place(None, k_cache, late * rows, late, out_shape)
        k_out = place(k_out, kd, 0, me ^ 1, out_shape)
        v_out = place(None, v_cache, late * rows, late, out_shape)
        v_out = place(v_out, vd, 0, me ^ 1, out_shape)
        k_out = place(k_out, kx0, 0, me ^ 2, out_shape, 1, 0)
        k_out = place(k_out, kx1, 0, me ^ 2, out_shape, rows - 1, 1)
        k_out = add_tail(k_out, key_new)
        v_out = add_tail(v_out, value_new)
        k_out = place(k_out, ky, 0, me ^ 3, out_shape)
        v_out = place(v_out, vx, 0, me ^ 2, out_shape)
        v_out = place(v_out, vy0, 0, me ^ 3, out_shape, rows - 1, 0)
        v_out = place_last(v_out, vy1)
        return hidden_out, state_new, k_out, v_out

    batch_spec = P(('dp', 'sp'), None)
    head_spec = P(('dp', 'sp'), 'tp', None, None)
    cache_spec = P('dp', 'tp', 'sp', None)
    in_specs = (batch_spec, P('sp', 'dp', 'tp', None, None), cache_spec, cache_spec, P('tp'), P(None), P(None, None, 'tp'), P(None, 'tp'), P('tp'), P('tp', None), P(None), P(None, 'tp', None, None), P('tp', None))
    out_specs = (batch_spec, head_spec, head_spec, head_spec)
    return jax.shard_map(step, mesh=mesh, in_specs=in_specs, out_specs=out_specs, check_vma=False)
```

```python
import functools

import jax
import jax.numpy as jnp
from jax import lax
from jax.experimental import pallas as pl
from jax.experimental.pallas import tpu as pltpu
from jax.sharding import PartitionSpec as P


NORM_EPS = 1e-6
ROPE_BASE = 10000000.0
RES_ALPHA = 1.0
RES_BETA = 1.0
CACHE_EXTRA = 16


F32 = jnp.float32
BF16 = jnp.bfloat16


def rms_norm(vals_in, gain_vec):
    vals32 = vals_in.astype(F32)
    inv_rms = lax.rsqrt(jnp.mean(vals32 * vals32, axis=-1, keepdims=True) + NORM_EPS)
    return vals32 * inv_rms * gain_vec


def rotary(vals_in, position):
    rope_dim = vals_in.shape[-1] // 2
    half_dim = rope_dim // 2
    inv_freq = ROPE_BASE ** (-jnp.arange(0, rope_dim, 2, dtype=F32) / rope_dim)
    angles = position * inv_freq
    cosine = jnp.cos(angles)
    sine_vals = jnp.sin(angles)
    vals32 = vals_in.astype(F32)
    first_half = vals32[..., :half_dim]
    second_half = vals32[..., half_dim:rope_dim]
    return jnp.concatenate([first_half * cosine - second_half * sine_vals, second_half * cosine + first_half * sine_vals, vals32[..., rope_dim:]], axis=-1).astype(BF16)


def merge(out_a, stats_a, out_b, stats_b):
    top = jnp.maximum(stats_a[:, 0], stats_b[:, 0])
    scale_a = jnp.exp(stats_a[:, 0] - top)
    scale_b = jnp.exp(stats_b[:, 0] - top)
    total = stats_a[:, 1] * scale_a + stats_b[:, 1] * scale_b
    return out_a * scale_a[..., None] + out_b * scale_b[..., None], jnp.stack([top, total], axis=1)


def pack(out, stats):
    dim = out.shape[-1]
    tail = stats.reshape(-1, dim)
    return jnp.concatenate([out.reshape(-1, dim), jnp.pad(tail, ((0, 8 - tail.shape[0]), (0, 0)))])


def unpack(packed, heads, group):
    lines, dim = packed.shape[0] - 8, packed.shape[1]
    rows = lines // (heads * group)
    tail = packed[lines:lines + 2 * lines // dim]
    return packed[:lines].reshape(rows, heads, group, dim), tail.reshape(rows, 2, heads, group)


def partner(me, mask):
    if mask == 1:
        return me + 1 - 2 * lax.rem(me, 2)
    if mask == 2:
        return lax.rem(me + 2, 4)
    return 3 - me if mask == 3 else me


def grab_block(rows, mask, row, first_head, src_ref, out_ref, sem):
    first = rows * partner(lax.axis_index('sp'), mask) + row
    copy = pltpu.make_async_copy(src_ref.at[pl.ds(first, 1), pl.ds(first_head, out_ref.shape[1])], out_ref, sem)
    copy.start()
    copy.wait()


def grab(cache, rows, mask, row, first_head, heads):
    shape = (1, heads) + cache.shape[2:]
    return pl.pallas_call(
        functools.partial(grab_block, rows, mask, row, first_head),
        in_specs=[pl.BlockSpec(memory_space=pltpu.HBM)],
        out_specs=pl.BlockSpec(memory_space=pltpu.VMEM),
        out_shape=pltpu.VMEM(shape, cache.dtype),
        scratch_shapes=[pltpu.SemaphoreType.DMA],
        compiler_params=pltpu.CompilerParams(vmem_limit_bytes=62 * 1024 * 1024),
        name="grab",
    )(cache)


def place_block(count, own, mask, out_first, head_first, src_ref, *refs):
    out_ref, buf, in_sems, out_sems = refs[-4:]
    heads, length = src_ref.shape[1], src_ref.shape[2]
    me = lax.axis_index('sp')
    src_first = me * count if own else 0
    pos = pl.multiple_of(partner(me, mask) * length, length)
    reads, writes = [], []
    for i in range(count):
        for j in range(heads):
            n = i * heads + j
            reads.append(pltpu.make_async_copy(src_ref.at[src_first + i, j], buf.at[n], in_sems.at[n]))
            writes.append(pltpu.make_async_copy(buf.at[n], out_ref.at[out_first + i, head_first + j, pl.ds(pos, length)], out_sems.at[n]))
    for copy in reads:
        copy.start()
    for read, write in zip(reads, writes):
        read.wait()
        write.start()
    for copy in writes:
        copy.wait()


def place(total, block, mask, out_shape, own=False, out_first=0, head_first=0):
    count = out_shape[0] if own else block.shape[0]
    pieces = count * block.shape[1]
    operands = [block] if total is None else [block, total]
    nbytes = 2 * pieces * block.shape[2] * block.shape[3] * 2
    return pl.pallas_call(
        functools.partial(place_block, count, own, mask, out_first, head_first),
        in_specs=[pl.BlockSpec(memory_space=pltpu.HBM)] * len(operands),
        out_specs=pl.BlockSpec(memory_space=pltpu.HBM),
        out_shape=jax.ShapeDtypeStruct(out_shape, block.dtype),
        scratch_shapes=[pltpu.VMEM((pieces,) + block.shape[2:], block.dtype), pltpu.SemaphoreType.DMA((pieces,)), pltpu.SemaphoreType.DMA((pieces,))],
        input_output_aliases={} if total is None else {1: 0},
        compiler_params=pltpu.CompilerParams(vmem_limit_bytes=62 * 1024 * 1024),
        cost_estimate=pl.CostEstimate(flops=nbytes * 30, bytes_accessed=nbytes, transcendentals=0),
        name="place",
    )(*operands)


def write_block(mask, row, head, src_ref, total_ref, out_ref, sem):
    length = src_ref.shape[2]
    pos = total_ref.shape[2] - length if mask is None else pl.multiple_of(partner(lax.axis_index('sp'), mask) * length, length)
    copy = pltpu.make_async_copy(src_ref, out_ref.at[pl.ds(row, src_ref.shape[0]), pl.ds(head, src_ref.shape[1]), pl.ds(pos, length)], sem)
    copy.start()
    copy.wait()


def write(total, block, mask, row=0, head=0):
    return pl.pallas_call(
        functools.partial(write_block, mask, row, head),
        in_specs=[pl.BlockSpec(memory_space=pltpu.VMEM), pl.BlockSpec(memory_space=pltpu.HBM)],
        out_specs=pl.BlockSpec(memory_space=pltpu.HBM),
        out_shape=jax.ShapeDtypeStruct(total.shape, total.dtype),
        scratch_shapes=[pltpu.SemaphoreType.DMA],
        input_output_aliases={1: 0},
        compiler_params=pltpu.CompilerParams(vmem_limit_bytes=62 * 1024 * 1024),
        name="write",
    )(pltpu.with_memory_space_constraint(block, pltpu.VMEM), total)


def solution(mesh):
    seq_shards = mesh.shape['sp']
    tp_size = mesh.shape['tp']

    def send(value, mask):
        return lax.ppermute(value, 'sp', [(i, i ^ mask) for i in range(seq_shards)])

    def tp_sum(value):
        return value + lax.ppermute(value, 'tp', [(0, 1), (1, 0)])

    def step(tokens, states, k_cache, v_cache, slopes, lin_gain, w_lin_qkv, w_lin_gate, out_gain, w_lin_out, attn_gain, w_attn_in, w_attn_out):
        rows = tokens.shape[0]
        kv_dev = k_cache.shape[1]
        shard_len = k_cache.shape[2]
        head_dim = k_cache.shape[3]
        group = w_attn_in.shape[2] - 2
        heads_dev = slopes.shape[0]
        prompt_len = seq_shards * shard_len
        me = lax.axis_index('sp')

        def rows_of(value, mask, first=0, count=rows):
            return lax.dynamic_slice_in_dim(value, rows * (me ^ mask) + first, count, 0)

        kx0_rows = grab(k_cache, rows, 2, 0, 0, 1)
        kx0 = send(kx0_rows, 2)
        k_src, _ = lax.optimization_barrier((k_cache, kx0_rows))
        kx1_rows = grab(k_src, rows, 2, 0, 1, kv_dev - 1)
        kx1 = send(kx1_rows, 2)
        k_src, slopes_a, _ = lax.optimization_barrier((k_cache, slopes, kx1_rows))
        kx2_rows = rows_of(k_src, 2, 1, rows - 1)
        kx2 = send(kx2_rows, 2)

        own = states[0]
        offset = (shard_len * (seq_shards - 1 - me)).astype(F32)
        decay = jnp.exp(-slopes_a * offset)[None, :, None, None]
        sa_rows = rows_of(own, 3) * decay
        sb_rows = rows_of(own, 1) * decay
        sa = send(sa_rows, 1)
        sb = send(sb_rows, 1)

        normed = rms_norm(tokens, lin_gain).astype(BF16)
        lin_proj = jnp.einsum('bd,dkn->bkn', normed, w_lin_qkv, preferred_element_type=F32)
        act_vals = jax.nn.silu(lin_proj).astype(BF16).reshape(rows, 3, heads_dev, head_dim)

        part_x = rows_of(own, 2) * decay + sa
        sx = send(part_x, 2)

        k_src, v_src, _ = lax.optimization_barrier((k_cache, v_cache, part_x))
        ky_rows = rows_of(k_src, 3)
        kd_rows = rows_of(k_src, 1)
        vd_rows = rows_of(v_src, 1)
        vx_rows = rows_of(v_src, 2)
        vy0_rows = rows_of(v_src, 3, 0, rows - 1)
        last_row = rows_of(v_src, 3, rows - 1, 1)
        vy1_rows = last_row[:, :kv_dev - 1]
        vy2_rows = last_row[:, kv_dev - 1:]
        ky = send(ky_rows, 3)
        kd = send(kd_rows, 1)
        vd = send(vd_rows, 1)

        gate_vals = jax.nn.sigmoid(jnp.dot(normed, w_lin_gate, preferred_element_type=F32))
        gate_vals = lax.optimization_barrier(gate_vals)

        moved_state = rows_of(own, 0) * decay + sb + sx
        state_new = jnp.exp(-slopes)[None, :, None, None] * moved_state + jnp.einsum('bhd,bhe->bhde', act_vals[:, 1], act_vals[:, 2], preferred_element_type=F32)
        lin_attn = jnp.einsum('bhd,bhde->bhe', act_vals[:, 0].astype(F32), state_new).reshape(rows, heads_dev * head_dim)
        square_sum = tp_sum(jnp.sum(lin_attn * lin_attn, axis=-1, keepdims=True))
        inv_rms = lax.rsqrt(square_sum / (tp_size * heads_dev * head_dim) + NORM_EPS)
        mixed_out = (lin_attn * inv_rms * out_gain * gate_vals).astype(BF16)
        lin_out = jnp.dot(mixed_out, w_lin_out, preferred_element_type=F32)
        lin_out = tp_sum(lin_out)
        hidden = (RES_ALPHA * normed.astype(F32) + RES_BETA * lin_out).astype(BF16)
        normed_two = rms_norm(hidden, attn_gain).astype(BF16)
        attn_proj = jnp.einsum('bd,dkjn->bkjn', normed_two, w_attn_in, preferred_element_type=F32).astype(BF16)
        query_rot = rotary(attn_proj[:, :, :group], prompt_len)
        key_new = rotary(attn_proj[:, :, group], prompt_len)
        value_new = attn_proj[:, :, group + 1]

        qx = send(query_rot, 2)
        vx = send(vx_rows, 2)
        qd = send(jnp.stack([query_rot, qx]), 1)

        score_scale = head_dim ** -0.5
        order = jnp.arange(seq_shards) ^ me
        query_all = jnp.take(jnp.stack([query_rot, qd[0], qx, qd[1]]), order, axis=0).reshape(seq_shards * rows, kv_dev, group, head_dim)
        scores = jnp.einsum('bkgd,bktd->bkgt', query_all, k_cache, preferred_element_type=F32) * score_scale
        part_max = jnp.max(scores, axis=-1)
        probs = jnp.exp(scores - part_max[..., None])
        part_sum = jnp.sum(probs, axis=-1)
        part_out = jnp.einsum('bkgt,bktd->bkgd', probs.astype(BF16), v_cache, preferred_element_type=F32)
        stats = jnp.stack([part_max, part_sum], axis=1)

        pair = pack(jnp.concatenate([rows_of(part_out, 3), rows_of(part_out, 1)]), jnp.concatenate([rows_of(stats, 3), rows_of(stats, 1)]))
        pair_out, pair_stats = unpack(send(pair, 1), kv_dev, group)
        far = pack(*merge(rows_of(part_out, 2), rows_of(stats, 2), pair_out[:rows], pair_stats[:rows]))
        ax, axs = unpack(send(far, 2), kv_dev, group)
        vy0 = send(vy0_rows, 3)
        vy1 = send(vy1_rows, 3)
        vy2 = send(vy2_rows, 3)

        near_out, near_stats = merge(rows_of(part_out, 0), rows_of(stats, 0), pair_out[rows:], pair_stats[rows:])
        all_out, all_stats = merge(near_out, near_stats, ax, axs)
        new_score = jnp.einsum('clhe,cle->clh', query_rot, key_new, preferred_element_type=F32) * score_scale
        row_max = jnp.maximum(all_stats[:, 0], new_score)
        scale = jnp.exp(all_stats[:, 0] - row_max)
        new_prob = jnp.exp(new_score - row_max)
        prob_sum = all_stats[:, 1] * scale + new_prob
        weighted_sum = all_out * scale[..., None]
        weighted_sum = weighted_sum + new_prob.astype(BF16).astype(F32)[..., None] * value_new.astype(F32)[:, :, None, :]
        head_out = (weighted_sum / prob_sum[..., None]).astype(BF16).reshape(rows, kv_dev * group * head_dim)
        attn_out = jnp.dot(head_out, w_attn_out, preferred_element_type=F32)
        attn_out = tp_sum(attn_out)
        hidden_out = (RES_ALPHA * normed_two.astype(F32) + RES_BETA * attn_out).astype(BF16)

        out_shape = (rows, kv_dev, prompt_len + CACHE_EXTRA, head_dim)
        tail_zeros = jnp.zeros((rows, kv_dev, CACHE_EXTRA - 1, head_dim), BF16)
        k_src, v_src, _ = lax.optimization_barrier((k_cache, v_cache, part_x))

        def add_tail(total, new_row):
            return write(total, jnp.concatenate([new_row[:, :, None, :], tail_zeros], axis=2), None)

        k_out = place(None, k_src, 0, out_shape, own=True)
        k_out = place(k_out, kd, 1, out_shape)
        v_out = place(None, v_src, 0, out_shape, own=True)
        v_out = place(v_out, vd, 1, out_shape)
        k_out = place(k_out, kx2, 2, out_shape, out_first=1)
        k_out = place(k_out, kx0, 2, out_shape)
        k_out = place(k_out, kx1, 2, out_shape, head_first=1)
        k_out = add_tail(k_out, key_new)
        v_out = add_tail(v_out, value_new)
        k_out = place(k_out, ky, 3, out_shape)
        v_out = place(v_out, vx, 2, out_shape)
        v_out = place(v_out, vy0, 3, out_shape)
        v_out = place(v_out, vy1, 3, out_shape, out_first=rows - 1)
        v_out = write(v_out, vy2, 3, rows - 1, kv_dev - 1)
        return hidden_out, state_new, k_out, v_out

    batch_spec = P(('dp', 'sp'), None)
    head_spec = P(('dp', 'sp'), 'tp', None, None)
    cache_spec = P('dp', 'tp', 'sp', None)
    in_specs = (batch_spec, P('sp', 'dp', 'tp', None, None), cache_spec, cache_spec, P('tp'), P(None), P(None, None, 'tp'), P(None, 'tp'), P('tp'), P('tp', None), P(None), P(None, 'tp', None, None), P('tp', None))
    out_specs = (batch_spec, head_spec, head_spec, head_spec)
    return jax.shard_map(step, mesh=mesh, in_specs=in_specs, out_specs=out_specs, check_vma=False)
```

```python
import functools

import jax
import jax.numpy as jnp
from jax import lax
from jax.experimental import pallas as pl
from jax.experimental.pallas import tpu as pltpu
from jax.sharding import PartitionSpec as P


NORM_EPS = 1e-6
ROPE_BASE = 10000000.0
RES_ALPHA = 1.0
RES_BETA = 1.0
CACHE_EXTRA = 16


F32 = jnp.float32
BF16 = jnp.bfloat16


def rms_norm(vals_in, gain_vec):
    vals32 = vals_in.astype(F32)
    inv_rms = lax.rsqrt(jnp.mean(vals32 * vals32, axis=-1, keepdims=True) + NORM_EPS)
    return vals32 * inv_rms * gain_vec


def rotary(vals_in, position):
    rope_dim = vals_in.shape[-1] // 2
    half_dim = rope_dim // 2
    inv_freq = ROPE_BASE ** (-jnp.arange(0, rope_dim, 2, dtype=F32) / rope_dim)
    angles = position * inv_freq
    cosine = jnp.cos(angles)
    sine_vals = jnp.sin(angles)
    vals32 = vals_in.astype(F32)
    first_half = vals32[..., :half_dim]
    second_half = vals32[..., half_dim:rope_dim]
    return jnp.concatenate([first_half * cosine - second_half * sine_vals, second_half * cosine + first_half * sine_vals, vals32[..., rope_dim:]], axis=-1).astype(BF16)


def merge(out_a, stats_a, out_b, stats_b):
    top = jnp.maximum(stats_a[:, 0], stats_b[:, 0])
    scale_a = jnp.exp(stats_a[:, 0] - top)
    scale_b = jnp.exp(stats_b[:, 0] - top)
    total = stats_a[:, 1] * scale_a + stats_b[:, 1] * scale_b
    return out_a * scale_a[..., None] + out_b * scale_b[..., None], jnp.stack([top, total], axis=1)


def pack(out, stats):
    dim = out.shape[-1]
    tail = jnp.pad(stats.reshape(-1), (0, 8 * dim - stats.size)).reshape(8, dim)
    return jnp.concatenate([out.reshape(-1, dim), tail])


def unpack(packed, heads, group):
    lines, dim = packed.shape[0] - 8, packed.shape[1]
    rows = lines // (heads * group)
    tail = packed[lines:].reshape(-1)[:2 * lines]
    return packed[:lines].reshape(rows, heads, group, dim), tail.reshape(rows, 2, heads, group)


def attend(query, keys, values):
    scores = jnp.einsum('bkgd,bktd->bkgt', query, keys, preferred_element_type=F32) * query.shape[-1] ** -0.5
    top = jnp.max(scores, axis=-1)
    probs = jnp.exp(scores - top[..., None])
    out = jnp.einsum('bkgt,bktd->bkgd', probs.astype(BF16), values, preferred_element_type=F32)
    return out, jnp.stack([top, jnp.sum(probs, axis=-1)], axis=1)


def partner(me, mask):
    if mask == 1:
        return me + 1 - 2 * lax.rem(me, 2)
    if mask == 2:
        return lax.rem(me + 2, 4)
    return 3 - me if mask == 3 else me


def grab_block(rows, mask, row, first_head, src_ref, out_ref, sem):
    first = rows * partner(lax.axis_index('sp'), mask) + row
    copy = pltpu.make_async_copy(src_ref.at[pl.ds(first, 1), pl.ds(first_head, out_ref.shape[1])], out_ref, sem)
    copy.start()
    copy.wait()


def grab(cache, rows, mask, row, first_head, heads):
    shape = (1, heads) + cache.shape[2:]
    return pl.pallas_call(
        functools.partial(grab_block, rows, mask, row, first_head),
        in_specs=[pl.BlockSpec(memory_space=pltpu.HBM)],
        out_specs=pl.BlockSpec(memory_space=pltpu.VMEM),
        out_shape=pltpu.VMEM(shape, cache.dtype),
        scratch_shapes=[pltpu.SemaphoreType.DMA],
        compiler_params=pltpu.CompilerParams(vmem_limit_bytes=62 * 1024 * 1024),
        name="grab",
    )(cache)


def move_block(rows, source, target, src_ref, *refs):
    out_ref, buf, in_sems, out_sems = refs[-4:]
    pieces, heads, length = buf.shape[:3]
    me = lax.axis_index('sp')
    src_mask, src_row, src_head = source
    dst_mask, dst_row, dst_head = target
    src_row = src_row if src_mask is None else rows * partner(me, src_mask) + src_row
    pos = 0 if dst_mask is None else pl.multiple_of(partner(me, dst_mask) * length, length)
    reads, writes = [], []
    for n in range(pieces):
        reads.append(pltpu.make_async_copy(src_ref.at[src_row + n, pl.ds(src_head, heads)], buf.at[n], in_sems.at[n]))
        writes.append(pltpu.make_async_copy(buf.at[n], out_ref.at[dst_row + n, pl.ds(dst_head, heads), pl.ds(pos, length)], out_sems.at[n]))
    for copy in reads:
        copy.start()
    for read, write in zip(reads, writes):
        read.wait()
        write.start()
    for copy in writes:
        copy.wait()


def move(block, total, out_shape, count, heads, source, target, rows):
    operands = [block] if total is None else [block, total]
    length, dim = block.shape[2:]
    nbytes = 2 * count * heads * length * dim * 2
    return pl.pallas_call(
        functools.partial(move_block, rows, source, target),
        in_specs=[pl.BlockSpec(memory_space=pltpu.HBM)] * len(operands),
        out_specs=pl.BlockSpec(memory_space=pltpu.HBM),
        out_shape=jax.ShapeDtypeStruct(out_shape, block.dtype),
        scratch_shapes=[pltpu.VMEM((count, heads, length, dim), block.dtype), pltpu.SemaphoreType.DMA((count,)), pltpu.SemaphoreType.DMA((count,))],
        input_output_aliases={} if total is None else {1: 0},
        compiler_params=pltpu.CompilerParams(vmem_limit_bytes=62 * 1024 * 1024),
        cost_estimate=pl.CostEstimate(flops=nbytes * 30, bytes_accessed=nbytes, transcendentals=0),
        name="move",
    )(*operands)


def place(total, block, mask, out_shape, own=False, out_first=0, head_first=0):
    count = out_shape[0] if own else block.shape[0]
    return move(block, total, out_shape, count, block.shape[1], (0 if own else None, 0, 0), (mask, out_first, head_first), out_shape[0])


def cut(cache, rows, mask, first, count, head=0, heads=None):
    heads = cache.shape[1] if heads is None else heads
    return move(cache, None, (count, heads) + cache.shape[2:], count, heads, (mask, first, head), (None, 0, 0), rows)


def write_block(mask, row, head, src_ref, total_ref, out_ref, sem):
    length = src_ref.shape[2]
    pos = total_ref.shape[2] - length if mask is None else pl.multiple_of(partner(lax.axis_index('sp'), mask) * length, length)
    copy = pltpu.make_async_copy(src_ref, out_ref.at[pl.ds(row, src_ref.shape[0]), pl.ds(head, src_ref.shape[1]), pl.ds(pos, length)], sem)
    copy.start()
    copy.wait()


def write(total, block, mask, row=0, head=0):
    return pl.pallas_call(
        functools.partial(write_block, mask, row, head),
        in_specs=[pl.BlockSpec(memory_space=pltpu.VMEM), pl.BlockSpec(memory_space=pltpu.HBM)],
        out_specs=pl.BlockSpec(memory_space=pltpu.HBM),
        out_shape=jax.ShapeDtypeStruct(total.shape, total.dtype),
        scratch_shapes=[pltpu.SemaphoreType.DMA],
        input_output_aliases={1: 0},
        compiler_params=pltpu.CompilerParams(vmem_limit_bytes=62 * 1024 * 1024),
        name="write",
    )(pltpu.with_memory_space_constraint(block, pltpu.VMEM), total)


def solution(mesh):
    seq_shards = mesh.shape['sp']
    tp_size = mesh.shape['tp']

    def send(value, mask):
        return lax.ppermute(value, 'sp', [(i, i ^ mask) for i in range(seq_shards)])

    def tp_sum(value):
        return value + lax.ppermute(value, 'tp', [(0, 1), (1, 0)])

    def step(tokens, states, k_cache, v_cache, slopes, lin_gain, w_lin_qkv, w_lin_gate, out_gain, w_lin_out, attn_gain, w_attn_in, w_attn_out):
        rows = tokens.shape[0]
        kv_dev = k_cache.shape[1]
        shard_len = k_cache.shape[2]
        head_dim = k_cache.shape[3]
        group = w_attn_in.shape[2] - 2
        heads_dev = slopes.shape[0]
        prompt_len = seq_shards * shard_len
        me = lax.axis_index('sp')

        def rows_of(value, mask, first=0, count=rows):
            return lax.dynamic_slice_in_dim(value, rows * (me ^ mask) + first, count, 0)

        kx0_rows = grab(k_cache, rows, 2, 0, 0, 1)
        kx0 = send(kx0_rows, 2)
        k_src, _ = lax.optimization_barrier((k_cache, kx0_rows))
        kx1_rows = grab(k_src, rows, 2, 0, 1, kv_dev - 1)
        kx1 = send(kx1_rows, 2)
        k_src, slopes_a, _ = lax.optimization_barrier((k_cache, slopes, kx1_rows))
        kx2_rows = cut(k_src, rows, 2, 1, rows - 1)
        kx2 = send(kx2_rows, 2)

        own = states[0]
        offset = (shard_len * (seq_shards - 1 - me)).astype(F32)
        decay = jnp.exp(-slopes_a * offset)[None, :, None, None]
        sa_rows = rows_of(own, 3) * decay
        sb_rows = rows_of(own, 1) * decay
        sa = send(sa_rows, 1)
        sb = send(sb_rows, 1)

        normed = rms_norm(tokens, lin_gain).astype(BF16)
        lin_proj = jnp.einsum('bd,dkn->bkn', normed, w_lin_qkv, preferred_element_type=F32)
        act_vals = jax.nn.silu(lin_proj).astype(BF16).reshape(rows, 3, heads_dev, head_dim)

        part_x = rows_of(own, 2) * decay + sa
        sx = send(part_x, 2)

        k_src, v_src, _ = lax.optimization_barrier((k_cache, v_cache, part_x))
        ky_rows = cut(k_src, rows, 3, 1, rows - 1)
        ky0_rows = cut(k_src, rows, 3, 0, 1)
        kd_rows = cut(k_src, rows, 1, 0, rows)
        vd_rows = cut(v_src, rows, 1, 0, rows)
        vx_rows = cut(v_src, rows, 2, 1, rows - 1)
        vx0_rows = cut(v_src, rows, 2, 0, 1)
        vy_rows = cut(v_src, rows, 3, 1, rows - 1)
        vy0_rows = cut(v_src, rows, 3, 0, 1, 0, kv_dev - 1)
        vy1_rows = cut(v_src, rows, 3, 0, 1, kv_dev - 1, 1)
        ky0 = send(ky0_rows, 3)
        ky = send(ky_rows, 3)
        kd = send(kd_rows, 1)
        vd = send(vd_rows, 1)

        gate_vals = jax.nn.sigmoid(jnp.dot(normed, w_lin_gate, preferred_element_type=F32))
        gate_vals = lax.optimization_barrier(gate_vals)

        moved_state = rows_of(own, 0) * decay + sb + sx
        state_new = jnp.exp(-slopes)[None, :, None, None] * moved_state + jnp.einsum('bhd,bhe->bhde', act_vals[:, 1], act_vals[:, 2], preferred_element_type=F32)
        lin_attn = jnp.einsum('bhd,bhde->bhe', act_vals[:, 0].astype(F32), state_new).reshape(rows, heads_dev * head_dim)
        square_sum = tp_sum(jnp.sum(lin_attn * lin_attn, axis=-1, keepdims=True))
        inv_rms = lax.rsqrt(square_sum / (tp_size * heads_dev * head_dim) + NORM_EPS)
        mixed_out = (lin_attn * inv_rms * out_gain * gate_vals).astype(BF16)
        lin_out = jnp.dot(mixed_out, w_lin_out, preferred_element_type=F32)
        lin_out = tp_sum(lin_out)
        hidden = (RES_ALPHA * normed.astype(F32) + RES_BETA * lin_out).astype(BF16)
        normed_two = rms_norm(hidden, attn_gain).astype(BF16)
        attn_proj = jnp.einsum('bd,dkjn->bkjn', normed_two, w_attn_in, preferred_element_type=F32).astype(BF16)
        query_rot = rotary(attn_proj[:, :, :group], prompt_len)
        key_new = rotary(attn_proj[:, :, group], prompt_len)
        value_new = attn_proj[:, :, group + 1]

        qx = send(query_rot[:1], 2)
        vx = send(vx_rows, 2)
        qd = send(jnp.concatenate([query_rot, qx]), 1)

        order = jnp.arange(seq_shards) ^ me
        unused = jnp.zeros((rows - 1,) + query_rot.shape[1:], BF16)
        query_all = jnp.stack([query_rot, qd[:rows], jnp.concatenate([qx, unused]), jnp.concatenate([qd[rows:], unused])])
        query_all = jnp.take(query_all, order, axis=0).reshape(seq_shards * rows, kv_dev, group, head_dim)
        part_out, stats = attend(query_all, k_cache, v_cache)

        pair = pack(jnp.concatenate([rows_of(part_out, 3, 0, 1), rows_of(part_out, 1)]), jnp.concatenate([rows_of(stats, 3, 0, 1), rows_of(stats, 1)]))
        pair_out, pair_stats = unpack(send(pair, 1), kv_dev, group)
        far = pack(*merge(rows_of(part_out, 2, 0, 1), rows_of(stats, 2, 0, 1), pair_out[:1], pair_stats[:1]))
        ax, axs = unpack(send(far, 2), kv_dev, group)
        vy = send(vy_rows, 3)
        vx0 = send(vx0_rows, 2)
        vy0 = send(vy0_rows, 3)
        vy1 = send(vy1_rows, 3)

        home_x = attend(query_rot[1:], kx2, vx)
        home_y = attend(query_rot[1:], ky, vy)
        near_out, near_stats = merge(rows_of(part_out, 0), rows_of(stats, 0), pair_out[1:], pair_stats[1:])
        home_out, home_stats = merge(*home_x, *home_y)
        all_out, all_stats = merge(near_out, near_stats, jnp.concatenate([ax, home_out]), jnp.concatenate([axs, home_stats]))
        score_scale = head_dim ** -0.5
        new_score = jnp.einsum('clhe,cle->clh', query_rot, key_new, preferred_element_type=F32) * score_scale
        row_max = jnp.maximum(all_stats[:, 0], new_score)
        scale = jnp.exp(all_stats[:, 0] - row_max)
        new_prob = jnp.exp(new_score - row_max)
        prob_sum = all_stats[:, 1] * scale + new_prob
        weighted_sum = all_out * scale[..., None]
        weighted_sum = weighted_sum + new_prob.astype(BF16).astype(F32)[..., None] * value_new.astype(F32)[:, :, None, :]
        head_out = (weighted_sum / prob_sum[..., None]).astype(BF16).reshape(rows, kv_dev * group * head_dim)
        attn_out = jnp.dot(head_out, w_attn_out, preferred_element_type=F32)
        attn_out = tp_sum(attn_out)
        hidden_out = (RES_ALPHA * normed_two.astype(F32) + RES_BETA * attn_out).astype(BF16)

        out_shape = (rows, kv_dev, prompt_len + CACHE_EXTRA, head_dim)
        tail_zeros = jnp.zeros((rows, kv_dev, CACHE_EXTRA - 1, head_dim), BF16)
        k_src, v_src, _ = lax.optimization_barrier((k_cache, v_cache, part_x))

        def add_tail(total, new_row):
            return write(total, jnp.concatenate([new_row[:, :, None, :], tail_zeros], axis=2), None)

        k_out = place(None, k_src, 0, out_shape, own=True)
        k_out = place(k_out, kd, 1, out_shape)
        v_out = place(None, v_src, 0, out_shape, own=True)
        v_out = place(v_out, vd, 1, out_shape)
        k_out = place(k_out, kx2, 2, out_shape, out_first=1)
        k_out = place(k_out, kx0, 2, out_shape)
        k_out = place(k_out, kx1, 2, out_shape, head_first=1)
        k_out = add_tail(k_out, key_new)
        v_out = add_tail(v_out, value_new)
        k_out = place(k_out, ky0, 3, out_shape)
        k_out = place(k_out, ky, 3, out_shape, out_first=1)
        v_out = place(v_out, vx, 2, out_shape, out_first=1)
        v_out = place(v_out, vy, 3, out_shape, out_first=1)
        v_out = place(v_out, vx0, 2, out_shape)
        v_out = place(v_out, vy0, 3, out_shape)
        v_out = write(v_out, vy1, 3, 0, kv_dev - 1)
        return hidden_out, state_new, k_out, v_out

    batch_spec = P(('dp', 'sp'), None)
    head_spec = P(('dp', 'sp'), 'tp', None, None)
    cache_spec = P('dp', 'tp', 'sp', None)
    in_specs = (batch_spec, P('sp', 'dp', 'tp', None, None), cache_spec, cache_spec, P('tp'), P(None), P(None, None, 'tp'), P(None, 'tp'), P('tp'), P('tp', None), P(None), P(None, 'tp', None, None), P('tp', None))
    out_specs = (batch_spec, head_spec, head_spec, head_spec)
    return jax.shard_map(step, mesh=mesh, in_specs=in_specs, out_specs=out_specs, check_vma=False)
```

```python
import functools

import jax
import jax.numpy as jnp
from jax import lax
from jax.experimental import pallas as pl
from jax.experimental.pallas import tpu as pltpu
from jax.sharding import PartitionSpec as P


NORM_EPS = 1e-6
ROPE_BASE = 10000000.0
RES_ALPHA = 1.0
RES_BETA = 1.0
CACHE_EXTRA = 16


F32 = jnp.float32
BF16 = jnp.bfloat16


def rms_norm(vals_in, gain_vec):
    vals32 = vals_in.astype(F32)
    inv_rms = lax.rsqrt(jnp.mean(vals32 * vals32, axis=-1, keepdims=True) + NORM_EPS)
    return vals32 * inv_rms * gain_vec


def rotary(vals_in, position):
    rope_dim = vals_in.shape[-1] // 2
    half_dim = rope_dim // 2
    inv_freq = ROPE_BASE ** (-jnp.arange(0, rope_dim, 2, dtype=F32) / rope_dim)
    angles = position * inv_freq
    cosine = jnp.cos(angles)
    sine_vals = jnp.sin(angles)
    vals32 = vals_in.astype(F32)
    first_half = vals32[..., :half_dim]
    second_half = vals32[..., half_dim:rope_dim]
    return jnp.concatenate([first_half * cosine - second_half * sine_vals, second_half * cosine + first_half * sine_vals, vals32[..., rope_dim:]], axis=-1).astype(BF16)


def merge(out_a, stats_a, out_b, stats_b):
    top = jnp.maximum(stats_a[:, 0], stats_b[:, 0])
    scale_a = jnp.exp(stats_a[:, 0] - top)
    scale_b = jnp.exp(stats_b[:, 0] - top)
    total = stats_a[:, 1] * scale_a + stats_b[:, 1] * scale_b
    return out_a * scale_a[..., None] + out_b * scale_b[..., None], jnp.stack([top, total], axis=1)


def pack(out, stats):
    dim = out.shape[-1]
    tail = jnp.pad(stats.reshape(-1), (0, 8 * dim - stats.size)).reshape(8, dim)
    return jnp.concatenate([out.reshape(-1, dim), tail])


def unpack(packed, heads, group):
    lines, dim = packed.shape[0] - 8, packed.shape[1]
    rows = lines // (heads * group)
    tail = packed[lines:].reshape(-1)[:2 * lines]
    return packed[:lines].reshape(rows, heads, group, dim), tail.reshape(rows, 2, heads, group)


def attend(query, keys, values):
    scores = jnp.einsum('bkgd,bktd->bkgt', query, keys, preferred_element_type=F32) * query.shape[-1] ** -0.5
    top = jnp.max(scores, axis=-1)
    probs = jnp.exp(scores - top[..., None])
    out = jnp.einsum('bkgt,bktd->bkgd', probs.astype(BF16), values, preferred_element_type=F32)
    return out, jnp.stack([top, jnp.sum(probs, axis=-1)], axis=1)


def partner(me, mask):
    if mask == 1:
        return me + 1 - 2 * lax.rem(me, 2)
    if mask == 2:
        return lax.rem(me + 2, 4)
    return 3 - me if mask == 3 else me


def grab_block(rows, mask, row, first_head, src_ref, out_ref, sem):
    first = rows * partner(lax.axis_index('sp'), mask) + row
    copy = pltpu.make_async_copy(src_ref.at[pl.ds(first, 1), pl.ds(first_head, out_ref.shape[1])], out_ref, sem)
    copy.start()
    copy.wait()


def grab(cache, rows, mask, row, first_head, heads):
    shape = (1, heads) + cache.shape[2:]
    return pl.pallas_call(
        functools.partial(grab_block, rows, mask, row, first_head),
        in_specs=[pl.BlockSpec(memory_space=pltpu.HBM)],
        out_specs=pl.BlockSpec(memory_space=pltpu.VMEM),
        out_shape=pltpu.VMEM(shape, cache.dtype),
        scratch_shapes=[pltpu.SemaphoreType.DMA],
        compiler_params=pltpu.CompilerParams(vmem_limit_bytes=62 * 1024 * 1024),
        name="grab",
    )(cache)


def move_block(rows, jobs, n_src, n_out, aliased, *refs):
    srcs, outs = refs[:n_src], refs[n_src + aliased:n_src + aliased + n_out]
    bufs, in_sems, out_sems = refs[n_src + aliased + n_out:-2], refs[-2], refs[-1]
    me = lax.axis_index('sp')
    reads, writes = [], []
    for (src, source, out, target, count, heads), buf in zip(jobs, bufs):
        length = buf.shape[2]
        src_mask, src_row, src_head = source
        dst_mask, dst_row, dst_head = target
        src_row = src_row if src_mask is None else rows * partner(me, src_mask) + src_row
        pos = 0 if dst_mask is None else pl.multiple_of(partner(me, dst_mask) * length, length)
        for i in range(count):
            n = len(reads)
            reads.append(pltpu.make_async_copy(srcs[src].at[src_row + i, pl.ds(src_head, heads)], buf.at[i], in_sems.at[n]))
            writes.append(pltpu.make_async_copy(buf.at[i], outs[out].at[dst_row + i, pl.ds(dst_head, heads), pl.ds(pos, length)], out_sems.at[n]))
    for copy in reads:
        copy.start()
    for read, write in zip(reads, writes):
        read.wait()
        write.start()
    for copy in writes:
        copy.wait()


def move(srcs, jobs, out_shapes, rows, total=None):
    length, dim = srcs[0].shape[2:]
    dtype = srcs[0].dtype
    operands = list(srcs) if total is None else list(srcs) + [total]
    pieces = sum(job[4] for job in jobs)
    nbytes = 2 * sum(job[4] * job[5] for job in jobs) * length * dim * 2
    return pl.pallas_call(
        functools.partial(move_block, rows, jobs, len(srcs), len(out_shapes), len(operands) - len(srcs)),
        in_specs=[pl.BlockSpec(memory_space=pltpu.HBM)] * len(operands),
        out_specs=[pl.BlockSpec(memory_space=pltpu.HBM)] * len(out_shapes),
        out_shape=[jax.ShapeDtypeStruct(shape, dtype) for shape in out_shapes],
        scratch_shapes=[pltpu.VMEM((job[4], job[5], length, dim), dtype) for job in jobs] + [pltpu.SemaphoreType.DMA((pieces,)), pltpu.SemaphoreType.DMA((pieces,))],
        input_output_aliases={} if total is None else {len(srcs): 0},
        compiler_params=pltpu.CompilerParams(vmem_limit_bytes=62 * 1024 * 1024),
        cost_estimate=pl.CostEstimate(flops=nbytes * 30, bytes_accessed=nbytes, transcendentals=0),
        name="move",
    )(*operands)


def place(total, blocks, out_shape):
    rows = out_shape[0]
    jobs = []
    for n, (block, mask, row, head) in enumerate(blocks):
        own = mask == 0
        jobs.append((n, (0 if own else None, 0, 0), 0, (mask, row, head), rows if own else block.shape[0], block.shape[1]))
    return move([block[0] for block in blocks], jobs, [out_shape], rows, total)[0]


def cut(cache, rows, parts):
    jobs = [(0, (mask, first, head), n, (None, 0, 0), count, heads) for n, (mask, first, count, head, heads) in enumerate(parts)]
    return move([cache], jobs, [(part[2], part[4]) + cache.shape[2:] for part in parts], rows)


def write_block(mask, row, head, src_ref, total_ref, out_ref, sem):
    length = src_ref.shape[2]
    pos = total_ref.shape[2] - length if mask is None else pl.multiple_of(partner(lax.axis_index('sp'), mask) * length, length)
    copy = pltpu.make_async_copy(src_ref, out_ref.at[pl.ds(row, src_ref.shape[0]), pl.ds(head, src_ref.shape[1]), pl.ds(pos, length)], sem)
    copy.start()
    copy.wait()


def write(total, block, mask, row=0, head=0):
    return pl.pallas_call(
        functools.partial(write_block, mask, row, head),
        in_specs=[pl.BlockSpec(memory_space=pltpu.VMEM), pl.BlockSpec(memory_space=pltpu.HBM)],
        out_specs=pl.BlockSpec(memory_space=pltpu.HBM),
        out_shape=jax.ShapeDtypeStruct(total.shape, total.dtype),
        scratch_shapes=[pltpu.SemaphoreType.DMA],
        input_output_aliases={1: 0},
        compiler_params=pltpu.CompilerParams(vmem_limit_bytes=62 * 1024 * 1024),
        name="write",
    )(pltpu.with_memory_space_constraint(block, pltpu.VMEM), total)


def solution(mesh):
    seq_shards = mesh.shape['sp']
    tp_size = mesh.shape['tp']

    def send(value, mask):
        return lax.ppermute(value, 'sp', [(i, i ^ mask) for i in range(seq_shards)])

    def tp_sum(value):
        return value + lax.ppermute(value, 'tp', [(0, 1), (1, 0)])

    def step(tokens, states, k_cache, v_cache, slopes, lin_gain, w_lin_qkv, w_lin_gate, out_gain, w_lin_out, attn_gain, w_attn_in, w_attn_out):
        rows = tokens.shape[0]
        kv_dev = k_cache.shape[1]
        shard_len = k_cache.shape[2]
        head_dim = k_cache.shape[3]
        group = w_attn_in.shape[2] - 2
        heads_dev = slopes.shape[0]
        prompt_len = seq_shards * shard_len
        me = lax.axis_index('sp')

        def rows_of(value, mask, first=0, count=rows):
            return lax.dynamic_slice_in_dim(value, rows * (me ^ mask) + first, count, 0)

        kx0_rows = grab(k_cache, rows, 2, 0, 0, 1)
        kx0 = send(kx0_rows, 2)
        k_src, _ = lax.optimization_barrier((k_cache, kx0_rows))
        kx1_rows = grab(k_src, rows, 2, 0, 1, kv_dev - 1)
        kx1 = send(kx1_rows, 2)
        k_src, slopes_a, _ = lax.optimization_barrier((k_cache, slopes, kx1_rows))
        kx2_rows, = cut(k_src, rows, [(2, 1, rows - 1, 0, kv_dev)])
        kx2 = send(kx2_rows, 2)

        own = states[0]
        offset = (shard_len * (seq_shards - 1 - me)).astype(F32)
        decay = jnp.exp(-slopes_a * offset)[None, :, None, None]
        sa_rows = rows_of(own, 3) * decay
        sb_rows = rows_of(own, 1) * decay
        sa = send(sa_rows, 1)
        sb = send(sb_rows, 1)

        normed = rms_norm(tokens, lin_gain).astype(BF16)
        lin_proj = jnp.einsum('bd,dkn->bkn', normed, w_lin_qkv, preferred_element_type=F32)
        act_vals = jax.nn.silu(lin_proj).astype(BF16).reshape(rows, 3, heads_dev, head_dim)

        part_x = rows_of(own, 2) * decay + sa
        sx = send(part_x, 2)

        k_src, v_src, _ = lax.optimization_barrier((k_cache, v_cache, part_x))
        ky0_rows, ky_rows, kd_rows = cut(k_src, rows, [(3, 0, 1, 0, kv_dev), (3, 1, rows - 1, 0, kv_dev), (1, 0, rows, 0, kv_dev)])
        vd_rows, vx_rows, vy_rows, vx0_rows, vy0_rows, vy1_rows = cut(v_src, rows, [
            (1, 0, rows, 0, kv_dev),
            (2, 1, rows - 1, 0, kv_dev),
            (3, 1, rows - 1, 0, kv_dev),
            (2, 0, 1, 0, kv_dev),
            (3, 0, 1, 0, kv_dev - 1),
            (3, 0, 1, kv_dev - 1, 1),
        ])
        ky0 = send(ky0_rows, 3)
        ky = send(ky_rows, 3)
        kd = send(kd_rows, 1)
        vd = send(vd_rows, 1)

        gate_vals = jax.nn.sigmoid(jnp.dot(normed, w_lin_gate, preferred_element_type=F32))
        gate_vals = lax.optimization_barrier(gate_vals)

        moved_state = rows_of(own, 0) * decay + sb + sx
        state_new = jnp.exp(-slopes)[None, :, None, None] * moved_state + jnp.einsum('bhd,bhe->bhde', act_vals[:, 1], act_vals[:, 2], preferred_element_type=F32)
        lin_attn = jnp.einsum('bhd,bhde->bhe', act_vals[:, 0].astype(F32), state_new).reshape(rows, heads_dev * head_dim)
        square_sum = tp_sum(jnp.sum(lin_attn * lin_attn, axis=-1, keepdims=True))
        inv_rms = lax.rsqrt(square_sum / (tp_size * heads_dev * head_dim) + NORM_EPS)
        mixed_out = (lin_attn * inv_rms * out_gain * gate_vals).astype(BF16)
        lin_out = jnp.dot(mixed_out, w_lin_out, preferred_element_type=F32)
        lin_out = tp_sum(lin_out)
        hidden = (RES_ALPHA * normed.astype(F32) + RES_BETA * lin_out).astype(BF16)
        normed_two = rms_norm(hidden, attn_gain).astype(BF16)
        attn_proj = jnp.einsum('bd,dkjn->bkjn', normed_two, w_attn_in, preferred_element_type=F32).astype(BF16)
        query_rot = rotary(attn_proj[:, :, :group], prompt_len)
        key_new = rotary(attn_proj[:, :, group], prompt_len)
        value_new = attn_proj[:, :, group + 1]

        qx = send(query_rot[:1], 2)
        vx = send(vx_rows, 2)
        qd = send(jnp.concatenate([query_rot, qx]), 1)

        order = jnp.arange(seq_shards) ^ me
        unused = jnp.zeros((rows - 1,) + query_rot.shape[1:], BF16)
        query_all = jnp.stack([query_rot, qd[:rows], jnp.concatenate([qx, unused]), jnp.concatenate([qd[rows:], unused])])
        query_all = jnp.take(query_all, order, axis=0).reshape(seq_shards * rows, kv_dev, group, head_dim)
        part_out, stats = attend(query_all, k_cache, v_cache)

        pair = pack(jnp.concatenate([rows_of(part_out, 3, 0, 1), rows_of(part_out, 1)]), jnp.concatenate([rows_of(stats, 3, 0, 1), rows_of(stats, 1)]))
        pair_out, pair_stats = unpack(send(pair, 1), kv_dev, group)
        far = pack(*merge(rows_of(part_out, 2, 0, 1), rows_of(stats, 2, 0, 1), pair_out[:1], pair_stats[:1]))
        ax, axs = unpack(send(far, 2), kv_dev, group)
        vy = send(vy_rows, 3)
        vx0 = send(vx0_rows, 2)
        vy0 = send(vy0_rows, 3)
        vy1 = send(vy1_rows, 3)

        home_x = attend(query_rot[1:], kx2, vx)
        home_y = attend(query_rot[1:], ky, vy)
        near_out, near_stats = merge(rows_of(part_out, 0), rows_of(stats, 0), pair_out[1:], pair_stats[1:])
        home_out, home_stats = merge(*home_x, *home_y)
        all_out, all_stats = merge(near_out, near_stats, jnp.concatenate([ax, home_out]), jnp.concatenate([axs, home_stats]))
        score_scale = head_dim ** -0.5
        new_score = jnp.einsum('clhe,cle->clh', query_rot, key_new, preferred_element_type=F32) * score_scale
        row_max = jnp.maximum(all_stats[:, 0], new_score)
        scale = jnp.exp(all_stats[:, 0] - row_max)
        new_prob = jnp.exp(new_score - row_max)
        prob_sum = all_stats[:, 1] * scale + new_prob
        weighted_sum = all_out * scale[..., None]
        weighted_sum = weighted_sum + new_prob.astype(BF16).astype(F32)[..., None] * value_new.astype(F32)[:, :, None, :]
        head_out = (weighted_sum / prob_sum[..., None]).astype(BF16).reshape(rows, kv_dev * group * head_dim)
        attn_out = jnp.dot(head_out, w_attn_out, preferred_element_type=F32)
        attn_out = tp_sum(attn_out)
        hidden_out = (RES_ALPHA * normed_two.astype(F32) + RES_BETA * attn_out).astype(BF16)

        out_shape = (rows, kv_dev, prompt_len + CACHE_EXTRA, head_dim)
        tail_zeros = jnp.zeros((rows, kv_dev, CACHE_EXTRA - 1, head_dim), BF16)
        k_src, v_src, _ = lax.optimization_barrier((k_cache, v_cache, part_x))

        def add_tail(total, new_row):
            return write(total, jnp.concatenate([new_row[:, :, None, :], tail_zeros], axis=2), None)

        k_out = place(None, [(k_src, 0, 0, 0), (kd, 1, 0, 0), (kx0, 2, 0, 0), (kx1, 2, 0, 1), (kx2, 2, 1, 0)], out_shape)
        v_out = place(None, [(v_src, 0, 0, 0), (vd, 1, 0, 0)], out_shape)
        k_out = add_tail(k_out, key_new)
        v_out = add_tail(v_out, value_new)
        k_out = place(k_out, [(ky0, 3, 0, 0), (ky, 3, 1, 0)], out_shape)
        v_out = place(v_out, [(vx, 2, 1, 0), (vy, 3, 1, 0), (vx0, 2, 0, 0)], out_shape)
        v_out = place(v_out, [(vy0, 3, 0, 0)], out_shape)
        v_out = write(v_out, vy1, 3, 0, kv_dev - 1)
        return hidden_out, state_new, k_out, v_out

    batch_spec = P(('dp', 'sp'), None)
    head_spec = P(('dp', 'sp'), 'tp', None, None)
    cache_spec = P('dp', 'tp', 'sp', None)
    in_specs = (batch_spec, P('sp', 'dp', 'tp', None, None), cache_spec, cache_spec, P('tp'), P(None), P(None, None, 'tp'), P(None, 'tp'), P('tp'), P('tp', None), P(None), P(None, 'tp', None, None), P('tp', None))
    out_specs = (batch_spec, head_spec, head_spec, head_spec)
    return jax.shard_map(step, mesh=mesh, in_specs=in_specs, out_specs=out_specs, check_vma=False)
```

```python
import functools

import jax
import jax.numpy as jnp
from jax import lax
from jax.experimental import pallas as pl
from jax.experimental.pallas import tpu as pltpu
from jax.sharding import PartitionSpec as P


NORM_EPS = 1e-6
ROPE_BASE = 10000000.0
RES_ALPHA = 1.0
RES_BETA = 1.0
CACHE_EXTRA = 16


F32 = jnp.float32
BF16 = jnp.bfloat16


def rms_norm(vals_in, gain_vec):
    vals32 = vals_in.astype(F32)
    inv_rms = lax.rsqrt(jnp.mean(vals32 * vals32, axis=-1, keepdims=True) + NORM_EPS)
    return vals32 * inv_rms * gain_vec


def rotary(vals_in, position):
    rope_dim = vals_in.shape[-1] // 2
    half_dim = rope_dim // 2
    inv_freq = ROPE_BASE ** (-jnp.arange(0, rope_dim, 2, dtype=F32) / rope_dim)
    angles = position * inv_freq
    cosine = jnp.cos(angles)
    sine_vals = jnp.sin(angles)
    vals32 = vals_in.astype(F32)
    first_half = vals32[..., :half_dim]
    second_half = vals32[..., half_dim:rope_dim]
    return jnp.concatenate([first_half * cosine - second_half * sine_vals, second_half * cosine + first_half * sine_vals, vals32[..., rope_dim:]], axis=-1).astype(BF16)


def merge(out_a, stats_a, out_b, stats_b):
    top = jnp.maximum(stats_a[:, 0], stats_b[:, 0])
    scale_a = jnp.exp(stats_a[:, 0] - top)
    scale_b = jnp.exp(stats_b[:, 0] - top)
    total = stats_a[:, 1] * scale_a + stats_b[:, 1] * scale_b
    return out_a * scale_a[..., None] + out_b * scale_b[..., None], jnp.stack([top, total], axis=1)


def pack(out, stats):
    dim = out.shape[-1]
    tail = jnp.pad(stats.reshape(-1), (0, 8 * dim - stats.size)).reshape(8, dim)
    return jnp.concatenate([out.reshape(-1, dim), tail])


def unpack(packed, heads, group):
    lines, dim = packed.shape[0] - 8, packed.shape[1]
    rows = lines // (heads * group)
    tail = packed[lines:].reshape(-1)[:2 * lines]
    return packed[:lines].reshape(rows, heads, group, dim), tail.reshape(rows, 2, heads, group)


def attend(query, keys, values):
    scores = jnp.einsum('bkgd,bktd->bkgt', query, keys, preferred_element_type=F32) * query.shape[-1] ** -0.5
    top = jnp.max(scores, axis=-1)
    probs = jnp.exp(scores - top[..., None])
    out = jnp.einsum('bkgt,bktd->bkgd', probs.astype(BF16), values, preferred_element_type=F32)
    return out, jnp.stack([top, jnp.sum(probs, axis=-1)], axis=1)


def partner(me, mask):
    if mask == 1:
        return me + 1 - 2 * lax.rem(me, 2)
    if mask == 2:
        return lax.rem(me + 2, 4)
    return 3 - me if mask == 3 else me


def grab_block(rows, mask, row, first_head, src_ref, out_ref, sem):
    first = rows * partner(lax.axis_index('sp'), mask) + row
    copy = pltpu.make_async_copy(src_ref.at[pl.ds(first, 1), pl.ds(first_head, out_ref.shape[1])], out_ref, sem)
    copy.start()
    copy.wait()


def grab(cache, rows, mask, row, first_head, heads):
    shape = (1, heads) + cache.shape[2:]
    return pl.pallas_call(
        functools.partial(grab_block, rows, mask, row, first_head),
        in_specs=[pl.BlockSpec(memory_space=pltpu.HBM)],
        out_specs=pl.BlockSpec(memory_space=pltpu.VMEM),
        out_shape=pltpu.VMEM(shape, cache.dtype),
        scratch_shapes=[pltpu.SemaphoreType.DMA],
        compiler_params=pltpu.CompilerParams(vmem_limit_bytes=62 * 1024 * 1024),
        name="grab",
    )(cache)


def move_block(rows, jobs, n_src, n_out, aliased, *refs):
    srcs, outs = refs[:n_src], refs[n_src + aliased:n_src + aliased + n_out]
    bufs, in_sems, out_sems = refs[n_src + aliased + n_out:-2], refs[-2], refs[-1]
    me = lax.axis_index('sp')
    reads, writes = [], []
    for (src, source, out, target, count, heads), buf in zip(jobs, bufs):
        length = buf.shape[2]
        src_mask, src_row, src_head = source
        dst_mask, dst_row, dst_head = target
        src_row = src_row if src_mask is None else rows * partner(me, src_mask) + src_row
        pos = 0 if dst_mask is None else pl.multiple_of(partner(me, dst_mask) * length, length)
        for i in range(count):
            n = len(reads)
            reads.append(pltpu.make_async_copy(srcs[src].at[src_row + i, pl.ds(src_head, heads)], buf.at[i], in_sems.at[n]))
            writes.append(pltpu.make_async_copy(buf.at[i], outs[out].at[dst_row + i, pl.ds(dst_head, heads), pl.ds(pos, length)], out_sems.at[n]))
    for copy in reads:
        copy.start()
    for copy in reversed(reads):
        copy.wait()
    for copy in writes:
        copy.start()
    for copy in writes:
        copy.wait()


def move(srcs, jobs, out_shapes, rows, total=None):
    length, dim = srcs[0].shape[2:]
    dtype = srcs[0].dtype
    operands = list(srcs) if total is None else list(srcs) + [total]
    pieces = sum(job[4] for job in jobs)
    nbytes = 2 * sum(job[4] * job[5] for job in jobs) * length * dim * 2
    return pl.pallas_call(
        functools.partial(move_block, rows, jobs, len(srcs), len(out_shapes), len(operands) - len(srcs)),
        in_specs=[pl.BlockSpec(memory_space=pltpu.HBM)] * len(operands),
        out_specs=[pl.BlockSpec(memory_space=pltpu.HBM)] * len(out_shapes),
        out_shape=[jax.ShapeDtypeStruct(shape, dtype) for shape in out_shapes],
        scratch_shapes=[pltpu.VMEM((job[4], job[5], length, dim), dtype) for job in jobs] + [pltpu.SemaphoreType.DMA((pieces,)), pltpu.SemaphoreType.DMA((pieces,))],
        input_output_aliases={} if total is None else {len(srcs): 0},
        compiler_params=pltpu.CompilerParams(vmem_limit_bytes=62 * 1024 * 1024),
        cost_estimate=pl.CostEstimate(flops=nbytes * 30, bytes_accessed=nbytes, transcendentals=0),
        name="move",
    )(*operands)


def place(total, blocks, out_shape):
    rows = out_shape[0]
    jobs = []
    for n, (block, mask, row, head) in enumerate(blocks):
        own = mask == 0
        jobs.append((n, (0 if own else None, 0, 0), 0, (mask, row, head), rows if own else block.shape[0], block.shape[1]))
    return move([block[0] for block in blocks], jobs, [out_shape], rows, total)[0]


def cut(cache, rows, parts):
    jobs = [(0, (mask, first, head), n, (None, 0, 0), count, heads) for n, (mask, first, count, head, heads) in enumerate(parts)]
    return move([cache], jobs, [(part[2], part[4]) + cache.shape[2:] for part in parts], rows)


def write_block(mask, row, head, src_ref, total_ref, out_ref, sem):
    length = src_ref.shape[2]
    pos = total_ref.shape[2] - length if mask is None else pl.multiple_of(partner(lax.axis_index('sp'), mask) * length, length)
    copy = pltpu.make_async_copy(src_ref, out_ref.at[pl.ds(row, src_ref.shape[0]), pl.ds(head, src_ref.shape[1]), pl.ds(pos, length)], sem)
    copy.start()
    copy.wait()


def write(total, block, mask, row=0, head=0):
    return pl.pallas_call(
        functools.partial(write_block, mask, row, head),
        in_specs=[pl.BlockSpec(memory_space=pltpu.VMEM), pl.BlockSpec(memory_space=pltpu.HBM)],
        out_specs=pl.BlockSpec(memory_space=pltpu.HBM),
        out_shape=jax.ShapeDtypeStruct(total.shape, total.dtype),
        scratch_shapes=[pltpu.SemaphoreType.DMA],
        input_output_aliases={1: 0},
        compiler_params=pltpu.CompilerParams(vmem_limit_bytes=62 * 1024 * 1024),
        name="write",
    )(pltpu.with_memory_space_constraint(block, pltpu.VMEM), total)


def solution(mesh):
    seq_shards = mesh.shape['sp']
    tp_size = mesh.shape['tp']

    def send(value, mask):
        return lax.ppermute(value, 'sp', [(i, i ^ mask) for i in range(seq_shards)])

    def tp_sum(value):
        return value + lax.ppermute(value, 'tp', [(0, 1), (1, 0)])

    def step(tokens, states, k_cache, v_cache, slopes, lin_gain, w_lin_qkv, w_lin_gate, out_gain, w_lin_out, attn_gain, w_attn_in, w_attn_out):
        rows = tokens.shape[0]
        kv_dev = k_cache.shape[1]
        shard_len = k_cache.shape[2]
        head_dim = k_cache.shape[3]
        group = w_attn_in.shape[2] - 2
        heads_dev = slopes.shape[0]
        prompt_len = seq_shards * shard_len
        me = lax.axis_index('sp')

        def rows_of(value, mask, first=0, count=rows):
            return lax.dynamic_slice_in_dim(value, rows * (me ^ mask) + first, count, 0)

        kx0_rows = grab(k_cache, rows, 2, 0, 0, 1)
        kx0 = send(kx0_rows, 2)
        k_src, _ = lax.optimization_barrier((k_cache, kx0_rows))
        kx1_rows = grab(k_src, rows, 2, 0, 1, kv_dev - 1)
        kx1 = send(kx1_rows, 2)
        k_src, slopes_a, _ = lax.optimization_barrier((k_cache, slopes, kx1_rows))
        kx2_rows, = cut(k_src, rows, [(2, 1, rows - 1, 0, kv_dev)])
        kx2 = send(kx2_rows, 2)

        own = states[0]
        offset = (shard_len * (seq_shards - 1 - me)).astype(F32)
        decay = jnp.exp(-slopes_a * offset)[None, :, None, None]
        sa_rows = rows_of(own, 3) * decay
        sb_rows = rows_of(own, 1) * decay
        sa = send(sa_rows, 1)
        sb = send(sb_rows, 1)

        normed = rms_norm(tokens, lin_gain).astype(BF16)
        lin_proj = jnp.einsum('bd,dkn->bkn', normed, w_lin_qkv, preferred_element_type=F32)
        act_vals = jax.nn.silu(lin_proj).astype(BF16).reshape(rows, 3, heads_dev, head_dim)

        part_x = rows_of(own, 2) * decay + sa
        sx = send(part_x, 2)

        k_src, v_src, _ = lax.optimization_barrier((k_cache, v_cache, part_x))
        ky0_rows, ky_rows, kd_rows = cut(k_src, rows, [(3, 0, 1, 0, kv_dev), (3, 1, rows - 1, 0, kv_dev), (1, 0, rows, 0, kv_dev)])
        vd_rows, vx_rows, vy_rows, vx0_rows, vy0_rows, vy1_rows = cut(v_src, rows, [
            (1, 0, rows, 0, kv_dev),
            (2, 1, rows - 1, 0, kv_dev),
            (3, 1, rows - 1, 0, kv_dev),
            (2, 0, 1, 0, kv_dev),
            (3, 0, 1, 0, kv_dev - 1),
            (3, 0, 1, kv_dev - 1, 1),
        ])
        ky0 = send(ky0_rows, 3)
        ky = send(ky_rows, 3)
        kd = send(kd_rows, 1)
        vd = send(vd_rows, 1)

        gate_vals = jax.nn.sigmoid(jnp.dot(normed, w_lin_gate, preferred_element_type=F32))
        gate_vals = lax.optimization_barrier(gate_vals)

        moved_state = rows_of(own, 0) * decay + sb + sx
        state_new = jnp.exp(-slopes)[None, :, None, None] * moved_state + jnp.einsum('bhd,bhe->bhde', act_vals[:, 1], act_vals[:, 2], preferred_element_type=F32)
        lin_attn = jnp.einsum('bhd,bhde->bhe', act_vals[:, 0].astype(F32), state_new).reshape(rows, heads_dev * head_dim)
        square_sum = tp_sum(jnp.sum(lin_attn * lin_attn, axis=-1, keepdims=True))
        inv_rms = lax.rsqrt(square_sum / (tp_size * heads_dev * head_dim) + NORM_EPS)
        mixed_out = (lin_attn * inv_rms * out_gain * gate_vals).astype(BF16)
        lin_out = jnp.dot(mixed_out, w_lin_out, preferred_element_type=F32)
        lin_out = tp_sum(lin_out)
        hidden = (RES_ALPHA * normed.astype(F32) + RES_BETA * lin_out).astype(BF16)
        normed_two = rms_norm(hidden, attn_gain).astype(BF16)
        attn_proj = jnp.einsum('bd,dkjn->bkjn', normed_two, w_attn_in, preferred_element_type=F32).astype(BF16)
        query_rot = rotary(attn_proj[:, :, :group], prompt_len)
        key_new = rotary(attn_proj[:, :, group], prompt_len)
        value_new = attn_proj[:, :, group + 1]

        qx = send(query_rot[:1], 2)
        vx = send(vx_rows, 2)
        qd = send(jnp.concatenate([query_rot, qx]), 1)

        order = jnp.arange(seq_shards) ^ me
        unused = jnp.zeros((rows - 1,) + query_rot.shape[1:], BF16)
        query_all = jnp.stack([query_rot, qd[:rows], jnp.concatenate([qx, unused]), jnp.concatenate([qd[rows:], unused])])
        query_all = jnp.take(query_all, order, axis=0).reshape(seq_shards * rows, kv_dev, group, head_dim)
        part_out, stats = attend(query_all, k_cache, v_cache)

        pair = pack(jnp.concatenate([rows_of(part_out, 3, 0, 1), rows_of(part_out, 1)]), jnp.concatenate([rows_of(stats, 3, 0, 1), rows_of(stats, 1)]))
        pair_out, pair_stats = unpack(send(pair, 1), kv_dev, group)
        far = pack(*merge(rows_of(part_out, 2, 0, 1), rows_of(stats, 2, 0, 1), pair_out[:1], pair_stats[:1]))
        ax, axs = unpack(send(far, 2), kv_dev, group)
        vy = send(vy_rows, 3)
        vx0 = send(vx0_rows, 2)
        vy0 = send(vy0_rows, 3)
        vy1 = send(vy1_rows, 3)

        home_x = attend(query_rot[1:], kx2, vx)
        home_y = attend(query_rot[1:], ky, vy)
        near_out, near_stats = merge(rows_of(part_out, 0), rows_of(stats, 0), pair_out[1:], pair_stats[1:])
        home_out, home_stats = merge(*home_x, *home_y)
        all_out, all_stats = merge(near_out, near_stats, jnp.concatenate([ax, home_out]), jnp.concatenate([axs, home_stats]))
        score_scale = head_dim ** -0.5
        new_score = jnp.einsum('clhe,cle->clh', query_rot, key_new, preferred_element_type=F32) * score_scale
        row_max = jnp.maximum(all_stats[:, 0], new_score)
        scale = jnp.exp(all_stats[:, 0] - row_max)
        new_prob = jnp.exp(new_score - row_max)
        prob_sum = all_stats[:, 1] * scale + new_prob
        weighted_sum = all_out * scale[..., None]
        weighted_sum = weighted_sum + new_prob.astype(BF16).astype(F32)[..., None] * value_new.astype(F32)[:, :, None, :]
        head_out = (weighted_sum / prob_sum[..., None]).astype(BF16).reshape(rows, kv_dev * group * head_dim)
        attn_out = jnp.dot(head_out, w_attn_out, preferred_element_type=F32)
        attn_out = tp_sum(attn_out)
        hidden_out = (RES_ALPHA * normed_two.astype(F32) + RES_BETA * attn_out).astype(BF16)

        out_shape = (rows, kv_dev, prompt_len + CACHE_EXTRA, head_dim)
        tail_zeros = jnp.zeros((rows, kv_dev, CACHE_EXTRA - 1, head_dim), BF16)
        k_src, v_src, _ = lax.optimization_barrier((k_cache, v_cache, part_x))

        def add_tail(total, new_row):
            return write(total, jnp.concatenate([new_row[:, :, None, :], tail_zeros], axis=2), None)

        k_out = place(None, [(k_src, 0, 0, 0), (kd, 1, 0, 0), (kx0, 2, 0, 0), (kx1, 2, 0, 1), (kx2, 2, 1, 0)], out_shape)
        v_out = place(None, [(v_src, 0, 0, 0), (vd, 1, 0, 0)], out_shape)
        k_out = add_tail(k_out, key_new)
        v_out = add_tail(v_out, value_new)
        k_out = place(k_out, [(ky0, 3, 0, 0), (ky, 3, 1, 0)], out_shape)
        v_out = place(v_out, [(vx, 2, 1, 0), (vy, 3, 1, 0), (vx0, 2, 0, 0)], out_shape)
        v_out = place(v_out, [(vy0, 3, 0, 0)], out_shape)
        v_out = write(v_out, vy1, 3, 0, kv_dev - 1)
        return hidden_out, state_new, k_out, v_out

    batch_spec = P(('dp', 'sp'), None)
    head_spec = P(('dp', 'sp'), 'tp', None, None)
    cache_spec = P('dp', 'tp', 'sp', None)
    in_specs = (batch_spec, P('sp', 'dp', 'tp', None, None), cache_spec, cache_spec, P('tp'), P(None), P(None, None, 'tp'), P(None, 'tp'), P('tp'), P('tp', None), P(None), P(None, 'tp', None, None), P('tp', None))
    out_specs = (batch_spec, head_spec, head_spec, head_spec)
    return jax.shard_map(step, mesh=mesh, in_specs=in_specs, out_specs=out_specs, check_vma=False)
```

```python
import functools

import jax
import jax.numpy as jnp
from jax import lax
from jax.experimental import pallas as pl
from jax.experimental.pallas import tpu as pltpu
from jax.sharding import PartitionSpec as P


NORM_EPS = 1e-6
ROPE_BASE = 10000000.0
RES_ALPHA = 1.0
RES_BETA = 1.0
CACHE_EXTRA = 16


F32 = jnp.float32
BF16 = jnp.bfloat16


def rms_norm(vals_in, gain_vec):
    vals32 = vals_in.astype(F32)
    inv_rms = lax.rsqrt(jnp.mean(vals32 * vals32, axis=-1, keepdims=True) + NORM_EPS)
    return vals32 * inv_rms * gain_vec


def rotary(vals_in, position):
    rope_dim = vals_in.shape[-1] // 2
    half_dim = rope_dim // 2
    inv_freq = ROPE_BASE ** (-jnp.arange(0, rope_dim, 2, dtype=F32) / rope_dim)
    angles = position * inv_freq
    cosine = jnp.cos(angles)
    sine_vals = jnp.sin(angles)
    vals32 = vals_in.astype(F32)
    first_half = vals32[..., :half_dim]
    second_half = vals32[..., half_dim:rope_dim]
    return jnp.concatenate([first_half * cosine - second_half * sine_vals, second_half * cosine + first_half * sine_vals, vals32[..., rope_dim:]], axis=-1).astype(BF16)


def merge(out_a, stats_a, out_b, stats_b):
    top = jnp.maximum(stats_a[:, 0], stats_b[:, 0])
    scale_a = jnp.exp(stats_a[:, 0] - top)
    scale_b = jnp.exp(stats_b[:, 0] - top)
    total = stats_a[:, 1] * scale_a + stats_b[:, 1] * scale_b
    return out_a * scale_a[..., None] + out_b * scale_b[..., None], jnp.stack([top, total], axis=1)


def pack(out, stats):
    dim = out.shape[-1]
    tail = jnp.pad(stats.reshape(-1), (0, 8 * dim - stats.size)).reshape(8, dim)
    return jnp.concatenate([out.reshape(-1, dim), tail])


def unpack(packed, heads, group):
    lines, dim = packed.shape[0] - 8, packed.shape[1]
    rows = lines // (heads * group)
    tail = packed[lines:].reshape(-1)[:2 * lines]
    return packed[:lines].reshape(rows, heads, group, dim), tail.reshape(rows, 2, heads, group)


def attend(query, keys, values):
    scores = jnp.einsum('bkgd,bktd->bkgt', query, keys, preferred_element_type=F32) * query.shape[-1] ** -0.5
    top = jnp.max(scores, axis=-1)
    probs = jnp.exp(scores - top[..., None])
    out = jnp.einsum('bkgt,bktd->bkgd', probs.astype(BF16), values, preferred_element_type=F32)
    return out, jnp.stack([top, jnp.sum(probs, axis=-1)], axis=1)


def partner(me, mask):
    if mask == 1:
        return me + 1 - 2 * lax.rem(me, 2)
    if mask == 2:
        return lax.rem(me + 2, 4)
    return 3 - me if mask == 3 else me


def grab_block(rows, mask, row, first_head, src_ref, out_ref, sem):
    first = rows * partner(lax.axis_index('sp'), mask) + row
    copy = pltpu.make_async_copy(src_ref.at[pl.ds(first, 1), pl.ds(first_head, out_ref.shape[1])], out_ref, sem)
    copy.start()
    copy.wait()


def grab(cache, rows, mask, row, first_head, heads):
    shape = (1, heads) + cache.shape[2:]
    return pl.pallas_call(
        functools.partial(grab_block, rows, mask, row, first_head),
        in_specs=[pl.BlockSpec(memory_space=pltpu.HBM)],
        out_specs=pl.BlockSpec(memory_space=pltpu.VMEM),
        out_shape=pltpu.VMEM(shape, cache.dtype),
        scratch_shapes=[pltpu.SemaphoreType.DMA],
        compiler_params=pltpu.CompilerParams(vmem_limit_bytes=62 * 1024 * 1024),
        name="grab",
    )(cache)


def move_block(rows, jobs, n_src, n_out, aliased, *refs):
    srcs, outs = refs[:n_src], refs[n_src + aliased:n_src + aliased + n_out]
    bufs, in_sems, out_sems = refs[n_src + aliased + n_out:-2], refs[-2], refs[-1]
    me = lax.axis_index('sp')
    reads, writes = [], []
    for (src, source, out, target, count, heads), buf in zip(jobs, bufs):
        length = buf.shape[2]
        src_mask, src_row, src_head = source
        dst_mask, dst_row, dst_head = target
        src_row = src_row if src_mask is None else rows * partner(me, src_mask) + src_row
        pos = 0 if dst_mask is None else pl.multiple_of(partner(me, dst_mask) * length, length)
        for i in range(count):
            n = len(reads)
            reads.append(pltpu.make_async_copy(srcs[src].at[src_row + i, pl.ds(src_head, heads)], buf.at[i], in_sems.at[n]))
            writes.append(pltpu.make_async_copy(buf.at[i], outs[out].at[dst_row + i, pl.ds(dst_head, heads), pl.ds(pos, length)], out_sems.at[n]))
    for copy in reads:
        copy.start()
    for read, write in zip(reads, writes):
        read.wait()
        write.start()
    for copy in writes:
        copy.wait()


def move(srcs, jobs, out_shapes, rows, total=None):
    length, dim = srcs[0].shape[2:]
    dtype = srcs[0].dtype
    operands = list(srcs) if total is None else list(srcs) + [total]
    pieces = sum(job[4] for job in jobs)
    nbytes = 2 * sum(job[4] * job[5] for job in jobs) * length * dim * 2
    return pl.pallas_call(
        functools.partial(move_block, rows, jobs, len(srcs), len(out_shapes), len(operands) - len(srcs)),
        in_specs=[pl.BlockSpec(memory_space=pltpu.HBM)] * len(operands),
        out_specs=[pl.BlockSpec(memory_space=pltpu.HBM)] * len(out_shapes),
        out_shape=[jax.ShapeDtypeStruct(shape, dtype) for shape in out_shapes],
        scratch_shapes=[pltpu.VMEM((job[4], job[5], length, dim), dtype) for job in jobs] + [pltpu.SemaphoreType.DMA((pieces,)), pltpu.SemaphoreType.DMA((pieces,))],
        input_output_aliases={} if total is None else {len(srcs): 0},
        compiler_params=pltpu.CompilerParams(vmem_limit_bytes=62 * 1024 * 1024),
        cost_estimate=pl.CostEstimate(flops=nbytes * 30, bytes_accessed=nbytes, transcendentals=0),
        name="move",
    )(*operands)


def place(total, blocks, out_shape):
    rows = out_shape[0]
    jobs = []
    for n, (block, mask, row, head) in enumerate(blocks):
        own = mask == 0
        jobs.append((n, (0 if own else None, 0, 0), 0, (mask, row, head), rows if own else block.shape[0], block.shape[1]))
    return move([block[0] for block in blocks], jobs, [out_shape], rows, total)[0]


def cut(cache, rows, parts):
    jobs = [(0, (mask, first, head), n, (None, 0, 0), count, heads) for n, (mask, first, count, head, heads) in enumerate(parts)]
    return move([cache], jobs, [(part[2], part[4]) + cache.shape[2:] for part in parts], rows)


def write_block(mask, row, head, span, offset, src_ref, total_ref, out_ref, sem):
    length = src_ref.shape[2]
    pos = total_ref.shape[2] - length if mask is None else pl.multiple_of(partner(lax.axis_index('sp'), mask) * span + offset, 256)
    copy = pltpu.make_async_copy(src_ref, out_ref.at[pl.ds(row, src_ref.shape[0]), pl.ds(head, src_ref.shape[1]), pl.ds(pos, length)], sem)
    copy.start()
    copy.wait()


def write(total, block, mask, row=0, head=0, span=0, offset=0):
    return pl.pallas_call(
        functools.partial(write_block, mask, row, head, span, offset),
        in_specs=[pl.BlockSpec(memory_space=pltpu.VMEM), pl.BlockSpec(memory_space=pltpu.HBM)],
        out_specs=pl.BlockSpec(memory_space=pltpu.HBM),
        out_shape=jax.ShapeDtypeStruct(total.shape, total.dtype),
        scratch_shapes=[pltpu.SemaphoreType.DMA],
        input_output_aliases={1: 0},
        compiler_params=pltpu.CompilerParams(vmem_limit_bytes=62 * 1024 * 1024),
        name="write",
    )(pltpu.with_memory_space_constraint(block, pltpu.VMEM), total)


def solution(mesh):
    seq_shards = mesh.shape['sp']
    tp_size = mesh.shape['tp']

    def send(value, mask):
        return lax.ppermute(value, 'sp', [(i, i ^ mask) for i in range(seq_shards)])

    def tp_sum(value):
        return value + lax.ppermute(value, 'tp', [(0, 1), (1, 0)])

    def step(tokens, states, k_cache, v_cache, slopes, lin_gain, w_lin_qkv, w_lin_gate, out_gain, w_lin_out, attn_gain, w_attn_in, w_attn_out):
        rows = tokens.shape[0]
        kv_dev = k_cache.shape[1]
        shard_len = k_cache.shape[2]
        head_dim = k_cache.shape[3]
        group = w_attn_in.shape[2] - 2
        heads_dev = slopes.shape[0]
        prompt_len = seq_shards * shard_len
        me = lax.axis_index('sp')

        def rows_of(value, mask, first=0, count=rows):
            return lax.dynamic_slice_in_dim(value, rows * (me ^ mask) + first, count, 0)

        kx0_rows = grab(k_cache, rows, 2, 0, 0, 1)
        kx0 = send(kx0_rows, 2)
        k_src, _ = lax.optimization_barrier((k_cache, kx0_rows))
        kx1_rows = grab(k_src, rows, 2, 0, 1, kv_dev - 1)
        kx1 = send(kx1_rows, 2)
        k_src, slopes_a, _ = lax.optimization_barrier((k_cache, slopes, kx1_rows))
        kx2_rows, = cut(k_src, rows, [(2, 1, rows - 1, 0, kv_dev)])
        kx2 = send(kx2_rows, 2)

        own = states[0]
        offset = (shard_len * (seq_shards - 1 - me)).astype(F32)
        decay = jnp.exp(-slopes_a * offset)[None, :, None, None]
        sa_rows = rows_of(own, 3) * decay
        sb_rows = rows_of(own, 1) * decay
        sa = send(sa_rows, 1)
        sb = send(sb_rows, 1)

        normed = rms_norm(tokens, lin_gain).astype(BF16)
        lin_proj = jnp.einsum('bd,dkn->bkn', normed, w_lin_qkv, preferred_element_type=F32)
        act_vals = jax.nn.silu(lin_proj).astype(BF16).reshape(rows, 3, heads_dev, head_dim)

        part_x = rows_of(own, 2) * decay + sa
        sx = send(part_x, 2)

        k_src, v_src, _ = lax.optimization_barrier((k_cache, v_cache, part_x))
        ky0_rows, ky_rows, kd_rows = cut(k_src, rows, [(3, 0, 1, 0, kv_dev), (3, 1, rows - 1, 0, kv_dev), (1, 0, rows, 0, kv_dev)])
        vd_rows, vx_rows, vy_rows, vx0_rows, vy0_rows, vy1_rows = cut(v_src, rows, [
            (1, 0, rows, 0, kv_dev),
            (2, 1, rows - 1, 0, kv_dev),
            (3, 1, rows - 1, 0, kv_dev),
            (2, 0, 1, 0, kv_dev),
            (3, 0, 1, 0, kv_dev - 1),
            (3, 0, 1, kv_dev - 1, 1),
        ])
        early = shard_len // 2
        vy2_rows = vy1_rows[:, :, early:]
        vy1_rows = vy1_rows[:, :, :early]
        ky0 = send(ky0_rows, 3)
        ky = send(ky_rows, 3)
        kd = send(kd_rows, 1)
        vd = send(vd_rows, 1)

        gate_vals = jax.nn.sigmoid(jnp.dot(normed, w_lin_gate, preferred_element_type=F32))
        gate_vals = lax.optimization_barrier(gate_vals)

        moved_state = rows_of(own, 0) * decay + sb + sx
        state_new = jnp.exp(-slopes)[None, :, None, None] * moved_state + jnp.einsum('bhd,bhe->bhde', act_vals[:, 1], act_vals[:, 2], preferred_element_type=F32)
        lin_attn = jnp.einsum('bhd,bhde->bhe', act_vals[:, 0].astype(F32), state_new).reshape(rows, heads_dev * head_dim)
        square_sum = tp_sum(jnp.sum(lin_attn * lin_attn, axis=-1, keepdims=True))
        inv_rms = lax.rsqrt(square_sum / (tp_size * heads_dev * head_dim) + NORM_EPS)
        mixed_out = (lin_attn * inv_rms * out_gain * gate_vals).astype(BF16)
        lin_out = jnp.dot(mixed_out, w_lin_out, preferred_element_type=F32)
        lin_out = tp_sum(lin_out)
        hidden = (RES_ALPHA * normed.astype(F32) + RES_BETA * lin_out).astype(BF16)
        normed_two = rms_norm(hidden, attn_gain).astype(BF16)
        attn_proj = jnp.einsum('bd,dkjn->bkjn', normed_two, w_attn_in, preferred_element_type=F32).astype(BF16)
        query_rot = rotary(attn_proj[:, :, :group], prompt_len)
        key_new = rotary(attn_proj[:, :, group], prompt_len)
        value_new = attn_proj[:, :, group + 1]

        qx = send(query_rot[:1], 2)
        vx = send(vx_rows, 2)
        qd = send(jnp.concatenate([query_rot, qx]), 1)

        order = jnp.arange(seq_shards) ^ me
        unused = jnp.zeros((rows - 1,) + query_rot.shape[1:], BF16)
        query_all = jnp.stack([query_rot, qd[:rows], jnp.concatenate([qx, unused]), jnp.concatenate([qd[rows:], unused])])
        query_all = jnp.take(query_all, order, axis=0).reshape(seq_shards * rows, kv_dev, group, head_dim)
        part_out, stats = attend(query_all, k_cache, v_cache)

        pair = pack(jnp.concatenate([rows_of(part_out, 3, 0, 1), rows_of(part_out, 1)]), jnp.concatenate([rows_of(stats, 3, 0, 1), rows_of(stats, 1)]))
        pair_out, pair_stats = unpack(send(pair, 1), kv_dev, group)
        far = pack(*merge(rows_of(part_out, 2, 0, 1), rows_of(stats, 2, 0, 1), pair_out[:1], pair_stats[:1]))
        ax, axs = unpack(send(far, 2), kv_dev, group)
        vy = send(vy_rows, 3)
        vx0 = send(vx0_rows, 2)
        vy0 = send(vy0_rows, 3)
        vy1 = send(vy1_rows, 3)
        vy2 = send(vy2_rows, 3)

        home_x = attend(query_rot[1:], kx2, vx)
        home_y = attend(query_rot[1:], ky, vy)
        near_out, near_stats = merge(rows_of(part_out, 0), rows_of(stats, 0), pair_out[1:], pair_stats[1:])
        home_out, home_stats = merge(*home_x, *home_y)
        all_out, all_stats = merge(near_out, near_stats, jnp.concatenate([ax, home_out]), jnp.concatenate([axs, home_stats]))
        score_scale = head_dim ** -0.5
        new_score = jnp.einsum('clhe,cle->clh', query_rot, key_new, preferred_element_type=F32) * score_scale
        row_max = jnp.maximum(all_stats[:, 0], new_score)
        scale = jnp.exp(all_stats[:, 0] - row_max)
        new_prob = jnp.exp(new_score - row_max)
        prob_sum = all_stats[:, 1] * scale + new_prob
        weighted_sum = all_out * scale[..., None]
        weighted_sum = weighted_sum + new_prob.astype(BF16).astype(F32)[..., None] * value_new.astype(F32)[:, :, None, :]
        head_out = (weighted_sum / prob_sum[..., None]).astype(BF16).reshape(rows, kv_dev * group * head_dim)
        attn_out = jnp.dot(head_out, w_attn_out, preferred_element_type=F32)
        attn_out = tp_sum(attn_out)
        hidden_out = (RES_ALPHA * normed_two.astype(F32) + RES_BETA * attn_out).astype(BF16)

        out_shape = (rows, kv_dev, prompt_len + CACHE_EXTRA, head_dim)
        tail_zeros = jnp.zeros((rows, kv_dev, CACHE_EXTRA - 1, head_dim), BF16)
        k_src, v_src, _ = lax.optimization_barrier((k_cache, v_cache, part_x))

        def add_tail(total, new_row):
            return write(total, jnp.concatenate([new_row[:, :, None, :], tail_zeros], axis=2), None)

        k_out = place(None, [(k_src, 0, 0, 0), (kd, 1, 0, 0), (kx0, 2, 0, 0), (kx1, 2, 0, 1), (kx2, 2, 1, 0)], out_shape)
        v_out = place(None, [(v_src, 0, 0, 0), (vd, 1, 0, 0)], out_shape)
        k_out = add_tail(k_out, key_new)
        v_out = add_tail(v_out, value_new)
        k_out = place(k_out, [(ky0, 3, 0, 0), (ky, 3, 1, 0)], out_shape)
        v_out = place(v_out, [(vx, 2, 1, 0), (vy, 3, 1, 0), (vx0, 2, 0, 0)], out_shape)
        v_out = place(v_out, [(vy0, 3, 0, 0)], out_shape)
        v_out = write(v_out, vy1, 3, 0, kv_dev - 1, shard_len)
        v_out = write(v_out, vy2, 3, 0, kv_dev - 1, shard_len, early)
        return hidden_out, state_new, k_out, v_out

    batch_spec = P(('dp', 'sp'), None)
    head_spec = P(('dp', 'sp'), 'tp', None, None)
    cache_spec = P('dp', 'tp', 'sp', None)
    in_specs = (batch_spec, P('sp', 'dp', 'tp', None, None), cache_spec, cache_spec, P('tp'), P(None), P(None, None, 'tp'), P(None, 'tp'), P('tp'), P('tp', None), P(None), P(None, 'tp', None, None), P('tp', None))
    out_specs = (batch_spec, head_spec, head_spec, head_spec)
    return jax.shard_map(step, mesh=mesh, in_specs=in_specs, out_specs=out_specs, check_vma=False)
```
